32 devices in a mesh: member: 2 (over y), win: 4 (over z), seq: 4 (over x, core).
Axes of the slice: x: 2, y: 2, z: 4, core: 2. Of those that a mesh axis runs over, the one named last changes fastest.
Arguments:
- pixel_grid_input: bfloat16 [8, 8, 4, 64, 1536], P(('member', 'win'), None, 'seq'), parts along dimension 0, may hold values from -6 to 6
- mask_zone_labeling: int32 [8, 32, 64], P(('member', 'win')), parts along dimension 0, may hold values from 0 to 8, as said below
- standardize_multiplier: float32 [1536], replicated, may hold values from 0.25 to 1.75
- standardize_offset_vector: float32 [1536], replicated, may hold values from -3 to 3
- triple_projection_matrix: bfloat16 [3, 1536, 1536], P(None, None, 'seq'), may hold values from -0.15625 to 0.15625
- logit_scaling_per_part: float32 [16], P('seq'), may hold values from 1 to 45
- final_projection_matrix: bfloat16 [1536, 1536], P('seq'), may hold values from -0.15625 to 0.15625
Outputs:
- mixed: bfloat16 [8, 8, 4, 64, 1536], P(('member', 'win'), None, 'seq'), parts along dimension 0
The draws below stay inside these ranges and needn't reach their ends.
There are 2 independent parts, one for each index of `member`. The reference program is written for one: setup_inputs(seed, part) draws one part's arguments, and reference() takes and returns one part's arrays. A program takes and returns all parts, laid end to end along the dimension named above; an argument that names none is the same for every part. Nothing has to cross between parts.
Inputs may be any that keep to these rules, and one draw needn't show every extreme that they name: `mask_zone_labeling`: region is 3 * (row band) + (column band) of the pixel on the rolled grid: the row band is 0 in the first 32 rows, 1 in the next rows and 2 in the last few rows, whose count is drawn once for each member from 4 to 27; the column bands are cut the same way within the last 32 columns of the grid, with a count drawn apart. Only windows in the last window row or the last window column of the grid hold more than one region.
All inputs are finite; a program needn't handle non-finite values.
Results may differ from the reference program's by a relative error of at most 0.0065.
The reference program's roundings to bfloat16 on the way count: a program that leaves them out, or rounds other values in their place, can miss the bound.
Values may be sent and summed in bfloat16 or wider, within the bound.
A program may use at most 64 MiB of HBM per device.

```python
import math
import jax
import jax.numpy as jnp
from jax import lax

D = 1536
HEADS = 16
CHANNEL_PER_PART = 96
WS = 32
WCD = 2
SHIFT = 16
LANES = 4
AROWS = 8
COLS = 64
N_WIN = 4


def draw_logit_scaling_per_part(key, part):
    logs = jax.random.uniform(key, (HEADS,), jnp.float32, 0.0, jnp.log(6.0))
    return jnp.exp(logs)


def draw_mask_zone_labeling(key, part):
    cuts = jax.random.randint(jax.random.fold_in(key, 17), (2,), 4, WS - 4)
    row_cut = cuts[0]
    col_cut = cuts[1]
    grid_rows = 2 * WS
    grid_width = N_WIN // 2 * COLS
    block_index = lax.broadcasted_iota(jnp.int32, (N_WIN, WS, COLS), 0)
    inner_row = lax.broadcasted_iota(jnp.int32, (N_WIN, WS, COLS), 1)
    inner_col = lax.broadcasted_iota(jnp.int32, (N_WIN, WS, COLS), 2)
    grid_row = block_index % 2 * WS + inner_row
    grid_col = block_index // 2 * COLS + inner_col
    row_band = jnp.where(grid_row < WS, 0, jnp.where(grid_row < grid_rows - row_cut, 1, 2))
    col_band = jnp.where(grid_col < grid_width - WS, 0, jnp.where(grid_col < grid_width - col_cut, 1, 2))
    return (3 * row_band + col_band).astype(jnp.int32)


def block_levels(own_key, shape, split, smallest, largest):
    loudness, own = 1.0, jax.random.fold_in(own_key, 6)
    for dim, blocks in split:
        heights = jnp.exp(jax.random.uniform(jax.random.fold_in(own, dim), (blocks,), jnp.float32, smallest / len(split), largest / len(split)))
        loudness = loudness * jnp.repeat(heights, shape[dim] // blocks).reshape([-1 if axis == dim else 1 for axis in range(len(shape))])
    return loudness


def scatter_about(key, shape, scale, bound, shards=(), kind=jnp.bfloat16):
    factor_of = block_levels(key, shape, shards, -0.22, 0.18) if shards else 1.0
    entries = jax.random.normal(key, shape, jnp.float32) * scale * factor_of
    return jnp.minimum(jnp.maximum(entries, -bound), bound).astype(kind)


def setup_inputs(seed: int = 0, part: int = 0) -> dict:
    key_list = jax.random.split(jax.random.key(seed), 8)
    own_keys = jax.random.split(jax.random.fold_in(key_list[7], part), 8)
    pixel_grid_input = scatter_about(own_keys[0], (N_WIN, AROWS, LANES, COLS, D), 1.0, 6.0, ((0, 4), (2, 4)))
    mask_zone_labeling = draw_mask_zone_labeling(jax.random.fold_in(jax.random.fold_in(key_list[7], part), 71), part)
    standardize_multiplier = jnp.clip(1.0 + 0.15 * jax.random.normal(key_list[2], (D,), jnp.float32), 0.25, 1.75)
    standardize_offset_vector = scatter_about(key_list[3], (D,), 0.5, 3.0, (), jnp.float32)
    triple_projection_matrix = scatter_about(key_list[4], (3, D, HEADS * CHANNEL_PER_PART), D ** -0.5, 0.15625, ((2, 4),))
    logit_scaling_per_part = draw_logit_scaling_per_part(jax.random.fold_in(key_list[7], 71), part)
    final_projection_matrix = scatter_about(key_list[6], (HEADS * CHANNEL_PER_PART, D), (HEADS * CHANNEL_PER_PART) ** -0.5, 0.15625, ((0, 4),))
    return dict(pixel_grid_input=pixel_grid_input, mask_zone_labeling=mask_zone_labeling, standardize_multiplier=standardize_multiplier, standardize_offset_vector=standardize_offset_vector, triple_projection_matrix=triple_projection_matrix, logit_scaling_per_part=logit_scaling_per_part, final_projection_matrix=final_projection_matrix)


def layer_norm(values_in, gain_vector, bias_vector):
    values = values_in.astype(jnp.float32)
    average = lax.optimization_barrier(jnp.mean(values, axis=-1, keepdims=True))
    centred = values - average
    variance = lax.optimization_barrier(jnp.mean(centred * centred, axis=-1, keepdims=True))
    return (centred * lax.rsqrt(variance + 1e-05) * gain_vector + bias_vector).astype(jnp.bfloat16)

def window_attend(triple, labels, logit_multiplier):
    queries = triple[0].astype(jnp.float32)
    keys_all = triple[1].astype(jnp.float32)
    values_all = triple[2].astype(jnp.float32)
    scores = jnp.einsum('hpe,hke->hpk', queries, keys_all) * logit_multiplier[:, None, None]
    same_region = labels[:, None] == labels[None, :]
    scores = jnp.where(same_region[None], scores, -1e+30)
    row_max = lax.optimization_barrier(jnp.max(scores, axis=-1, keepdims=True))
    numerators = jnp.exp(scores - row_max)
    probabilities = (numerators / lax.optimization_barrier(jnp.sum(numerators, axis=-1, keepdims=True))).astype(jnp.bfloat16)
    return jnp.einsum('hpk,hke->hpe', probabilities.astype(jnp.float32), values_all).astype(jnp.bfloat16)

def reference(pixel_grid_input, mask_zone_labeling, standardize_multiplier, standardize_offset_vector, triple_projection_matrix, logit_scaling_per_part, final_projection_matrix):
    grid_cols = N_WIN // 2
    blocks = pixel_grid_input.reshape(grid_cols, 2, WS, COLS, D)
    image = blocks.transpose(1, 2, 0, 3, 4).reshape(2 * WS, grid_cols * COLS, D)
    image = jnp.roll(image, (-SHIFT, -SHIFT), axis=(0, 1))
    blocks = image.reshape(2, WS, grid_cols, COLS, D).transpose(2, 0, 1, 3, 4).reshape(N_WIN, WS, COLS, D)
    windows = blocks.reshape(N_WIN, WS, WCD, WS, D).transpose(0, 2, 1, 3, 4).reshape(N_WIN * WCD, WS * WS, D)
    labels = mask_zone_labeling.reshape(N_WIN, WS, WCD, WS).transpose(0, 2, 1, 3).reshape(N_WIN * WCD, WS * WS)
    weights_qkv = triple_projection_matrix.astype(jnp.float32)
    logit_multiplier = logit_scaling_per_part / math.sqrt(CHANNEL_PER_PART)

    def one_window(pair):
        tokens, token_region_labels = pair
        normed = layer_norm(tokens, standardize_multiplier, standardize_offset_vector)
        triple = jnp.einsum('pd,tdc->tpc', normed.astype(jnp.float32), weights_qkv).astype(jnp.bfloat16)
        triple = triple.reshape(3, WS * WS, HEADS, CHANNEL_PER_PART).transpose(0, 2, 1, 3)
        heads_out = window_attend(triple, token_region_labels, logit_multiplier)
        joined = heads_out.transpose(1, 0, 2).reshape(WS * WS, HEADS * CHANNEL_PER_PART)
        attention_update = jnp.dot(joined, final_projection_matrix, preferred_element_type=jnp.float32)
        return (tokens.astype(jnp.float32) + attention_update).astype(jnp.bfloat16)
    result = lax.map(one_window, (windows, labels))
    result = result.reshape(N_WIN, WCD, WS, WS, D).transpose(0, 2, 1, 3, 4)
    return result.reshape(N_WIN, AROWS, LANES, COLS, D)
```

```python
import functools
import math

import jax
import jax.numpy as jnp
from jax import lax
from jax.experimental import pallas as pl
from jax.experimental.pallas import tpu as pltpu
from jax.sharding import PartitionSpec as P

CHANNEL_PER_PART = 96
PADDED = 128
WS = 32
HALF = WS // 2
LOG2E = 1.4426950408889634
MESH = pl.DeviceIdType.MESH


def xor(value, mask, bits):
    both = 0
    for b in range(bits):
        both = both + (1 << b) * ((value // (1 << b)) % 2) * ((mask // (1 << b)) % 2)
    return value + mask - 2 * both


def flip(value):
    return value + 1 - 2 * (value % 2)


def children(slot, lanes):
    low = lanes if slot == 0 else slot & -slot
    masks = [1 << b for b in reversed(range(lanes.bit_length() - 1))]
    return [slot | m for m in masks if m < low]


def layer_kernel(
    lanes,
    blocks,
    members,
    scale_ref,
    x_ref,
    label_ref,
    gain_ref,
    bias_ref,
    wqkv_ref,
    wout_ref,
    out_ref,
    pix,
    nrm,
    raw,
    wpad,
    wall,
    qkv,
    extq,
    extk,
    labt,
    att_out,
    att_in,
    acc,
    obuf,
    fetch_send,
    fetch_recv,
    norm_send,
    norm_recv,
    att_send,
    att_recv,
    w_send,
    w_recv,
    local_sem,
    out_sem,
):
    me = lax.axis_index("seq")
    win = lax.axis_index("win")
    member = lax.axis_index("member")
    bits = lanes.bit_length() - 1
    pieces, step, _, width = pix.shape
    rows = 2 * step
    group = step * HALF
    chunk = 4 * group
    window_count = pieces // 4
    head_width = att_out.shape[3]
    heads = head_width // CHANNEL_PER_PART
    cols = window_count * WS

    def at_seq(mask):
        return {"seq": xor(me, mask, bits)}

    def source(i):
        window, place, side = i // 4, (i // 2) % 2, i % 2
        first = window * WS + HALF + side * HALF
        span = pl.ds(step, step) if place == 0 else pl.ds(0, step)
        return place, first, x_ref.at[0, span, 0, pl.ds(first % cols, HALF), :]

    west = (win + blocks - 2) % blocks
    fetches = []
    locals_ = []
    for i in range(pieces):
        place, first, src = source(i)
        if place == 0 and first < cols:
            locals_.append(pltpu.make_async_copy(src, pix.at[i], fetch_recv.at[i]))
            continue
        if first < cols:
            to = flip(win)
        else:
            to = west if place == 0 else flip(west)
        fetches.append(
            pltpu.make_async_remote_copy(
                src_ref=src,
                dst_ref=pix.at[i],
                send_sem=fetch_send.at[i],
                recv_sem=fetch_recv.at[i],
                device_id={"win": to},
                device_id_type=MESH,
            )
        )

    def gather_copy(slot, i):
        parent = slot & (slot - 1)
        return pltpu.make_async_remote_copy(
            src_ref=nrm.at[parent, i],
            dst_ref=nrm.at[slot, i],
            send_sem=norm_send.at[slot, i],
            recv_sem=norm_recv.at[slot, i],
            device_id=at_seq(slot ^ parent),
            device_id_type=MESH,
        )

    def attended_copy(window, k):
        return pltpu.make_async_remote_copy(
            src_ref=att_out.at[window, k],
            dst_ref=att_in.at[window, k],
            send_sem=att_send.at[window, k],
            recv_sem=att_recv.at[window, k],
            device_id=at_seq(k),
            device_id_type=MESH,
        )

    w_copies = []

    def w_copy(src, dst, device):
        n = len(w_copies)
        copy = pltpu.make_async_remote_copy(
            src_ref=src,
            dst_ref=dst,
            send_sem=w_send.at[n],
            recv_sem=w_recv.at[n],
            device_id=device,
            device_id_type=MESH,
        )
        w_copies.append(copy)
        return copy

    def slot_rows(slot, start, count):
        if slot == 0:
            return wout_ref.at[pl.ds(start, count), :]
        return wall.at[slot, pl.ds(start, count), :]

    share_member, share_win = share_levels(members, blocks, head_width)
    part = head_width // (1 + share_member) // (1 + share_win)
    pair = part * (1 + share_member)
    w_stages = [[]]
    held = [0]
    masks = [1 << b for b in reversed(range(bits))]
    for mask in masks:
        grown = [k | mask for k in held]
        if mask == 1:
            direct = [w_copy(slot_rows(0, 0, head_width), wall.at[1], at_seq(1))]
            w_stages[0] += direct
            w_stages.append(
                [w_copy(wall.at[k], wall.at[k | 1], at_seq(1)) for k in held if k]
            )
        else:
            start = 0
            if share_win:
                start = (win % 2) * pair
            own = start
            if share_member:
                own = start + member * part
            own = pl.multiple_of(own, 16) if share_win or share_member else own
            stage = [
                w_copy(slot_rows(k, own, part), wall.at[k | mask, pl.ds(own, part), :], at_seq(mask))
                for k in held
            ]
            if held == [0]:
                w_stages[0] += stage
            else:
                w_stages.append(stage)
            if share_member:
                w_stages.append(
                    [
                        w_copy(
                            wall.at[k, pl.ds(own, part), :],
                            wall.at[k, pl.ds(own, part), :],
                            {"member": flip(member)},
                        )
                        for k in grown
                    ]
                )
            if share_win:
                begin = pl.multiple_of(start, 16)
                w_stages.append(
                    [
                        w_copy(
                            wall.at[k, pl.ds(begin, pair), :],
                            wall.at[k, pl.ds(begin, pair), :],
                            {"win": flip(win)},
                        )
                        for k in grown
                    ]
                )
        held = held + grown

    def w_stage(n):
        if 0 < n <= len(w_stages):
            for copy in w_stages[n - 1]:
                copy.wait_recv()
        if n < len(w_stages):
            for copy in w_stages[n]:
                copy.start()

    def norm(i):
        pltpu.make_async_copy(pix.at[i], pix.at[i], fetch_recv.at[i]).wait()
        gain = gain_ref[...]
        offset = bias_ref[...]
        for a in range(step):
            values = pix[i, a].astype(jnp.float32)
            average = jnp.mean(values, axis=-1, keepdims=True)
            centred = values - average
            variance = jnp.mean(centred * centred, axis=-1, keepdims=True)
            scaled = centred * lax.rsqrt(variance + 1e-05) * gain + offset
            nrm[0, i, a] = scaled.astype(jnp.bfloat16)

    def send(i):
        for slot in children(0, lanes):
            gather_copy(slot, i).start()

    inner = [k for k in range(1, lanes) if children(k, lanes)]
    inner.sort(key=lambda k: (bin(k).count("1"), -k))

    def forward(i):
        for k in inner:
            gather_copy(k, i).wait_recv()
            for slot in children(k, lanes):
                gather_copy(slot, i).start()

    def project_qkv(i):
        for k in range(1, lanes):
            if not children(k, lanes):
                gather_copy(k, i).wait_recv()
        window, place = i // 4, i % 4
        x = nrm[:, i].reshape(lanes * group, width)
        lane = lax.broadcasted_iota(jnp.int32, (lanes * group, PADDED), 1)
        ones = jnp.where(lane == CHANNEL_PER_PART, 1.0, 0.0).astype(jnp.bfloat16)
        q_extra = extq[i].reshape(lanes * group, PADDED)
        k_extra = extk[i].reshape(lanes * group, PADDED)
        for t, extra in enumerate((q_extra, k_extra, ones)):
            y = jnp.dot(x, wpad[t], preferred_element_type=jnp.float32).astype(jnp.bfloat16)
            for h in range(heads):
                part_y = y[:, h * PADDED : (h + 1) * PADDED] + extra
                qkv[t, window, :, place, :, h * PADDED : (h + 1) * PADDED] = part_y.reshape(
                    lanes, group, PADDED
                )

    def attend(window, k):
        for h in range(heads):
            span = slice(h * PADDED, (h + 1) * PADDED)
            tempered = scale_ref[h] * (LOG2E / math.sqrt(CHANNEL_PER_PART))
            q = qkv[0, window, k, :, :, span].reshape(chunk, PADDED)
            keys = qkv[1, window, :, :, :, span].reshape(lanes * chunk, PADDED)
            values = qkv[2, window, :, :, :, span].reshape(lanes * chunk, PADDED)
            scores = lax.dot_general(
                q, keys, (((1,), (1,)), ((), ())), preferred_element_type=jnp.float32
            )
            row_max = jnp.max(scores, axis=-1, keepdims=True)
            numerators = jnp.exp2((scores - row_max) * tempered).astype(jnp.bfloat16)
            summed = jnp.dot(numerators, values, preferred_element_type=jnp.float32)
            attended = summed / summed[:, CHANNEL_PER_PART : CHANNEL_PER_PART + 1]
            att_out[window, k, :, h * CHANNEL_PER_PART : (h + 1) * CHANNEL_PER_PART] = attended[
                :, :CHANNEL_PER_PART
            ].astype(jnp.bfloat16)

    def attend_and_send(window, k):
        attend(window, k)

        @pl.when(k > 0)
        def _():
            attended_copy(window, k).start()

    tile = 512 if width % 512 == 0 else width

    def emit(window):
        for piece in range(4):
            i = window * 4 + piece
            first = window * WS + (piece % 2) * HALF
            yield pltpu.make_async_copy(
                obuf.at[i],
                out_ref.at[0, pl.ds((piece // 2) * step, step), 0, pl.ds(first, HALF), :],
                out_sem.at[i],
            )

    def residual(window, columns):
        return pix[window * 4 : window * 4 + 4, :, :, columns].reshape(chunk, tile).astype(jnp.float32)

    def project_out(window, ready, late):
        for start in range(0, width, tile):
            columns = slice(start, start + tile)
            total = residual(window, columns)
            for k in ready:
                source_ref = att_out if k == 0 else att_in
                total += jnp.dot(
                    source_ref[window, k], wall[k, :, columns], preferred_element_type=jnp.float32
                )
            if late:
                acc[:, columns] = total
            else:
                obuf[window * 4 : window * 4 + 4, :, :, columns] = total.astype(
                    jnp.bfloat16
                ).reshape(4, step, HALF, tile)
        for n, k in enumerate(late):
            attended_copy(window, k).wait_recv()
            for start in range(0, width, tile):
                columns = slice(start, start + tile)
                total = acc[:, columns] + jnp.dot(
                    att_in[window, k], wall[k, :, columns], preferred_element_type=jnp.float32
                )
                if n + 1 < len(late):
                    acc[:, columns] = total
                else:
                    obuf[window * 4 : window * 4 + 4, :, :, columns] = total.astype(
                        jnp.bfloat16
                    ).reshape(4, step, HALF, tile)
        for copy in emit(window):
            copy.start()

    barrier = pltpu.get_barrier_semaphore()
    greeted = [at_seq(k) for k in range(1, lanes)]
    greeted += [{"win": flip(win)}, {"win": (win + 2) % blocks}, {"win": (flip(win) + 2) % blocks}]
    if share_member:
        greeted.append({"member": flip(member)})
    for device in greeted:
        pl.semaphore_signal(barrier, inc=1, device_id=device, device_id_type=MESH)
    for copy in locals_:
        copy.start()
    raw_copy = pltpu.make_async_copy(wqkv_ref, raw, local_sem.at[0])
    raw_copy.start()
    own_copy = pltpu.make_async_copy(wout_ref, wall.at[0], local_sem.at[1])
    own_copy.start()
    pl.semaphore_wait(barrier, len(greeted))
    for copy in fetches:
        copy.start()
    w_stage(0)

    @pl.loop(0, 2)
    def _(i):
        norm(i)
        send(i)

    labt[...] = jnp.zeros_like(labt)
    for k in range(lanes):
        lane_of = xor(me, k, bits)
        for a in range(rows):
            labt[a : a + 1, :cols] = label_ref[0, pl.ds(a * lanes + lane_of, 1), :].astype(jnp.float32)
        turned = jnp.transpose(labt[...])
        for i in range(pieces):
            first = (i // 4) * WS + (i % 2) * HALF
            for a in range(step):
                row = ((i // 2) % 2) * step + a
                label = turned[first : first + HALF, row : row + 1].astype(jnp.int32)
                lane = lax.broadcasted_iota(jnp.int32, (HALF, PADDED), 1) - CHANNEL_PER_PART
                same = lane == label
                extq[i, k, a] = jnp.where(same, 1.0, 0.0).astype(jnp.bfloat16)
                extk[i, k, a] = jnp.where(
                    jnp.logical_and(lane >= 0, jnp.logical_not(same)), -1e30, 0.0
                ).astype(jnp.bfloat16)

    raw_copy.wait()
    tall = width // 4

    @pl.loop(0, 12)
    def _(n):
        t, r = n // 4, pl.multiple_of((n % 4) * tall, tall)
        for h in range(heads):
            part_w = raw[t, pl.ds(r, tall), h * CHANNEL_PER_PART : (h + 1) * CHANNEL_PER_PART]
            empty = jnp.zeros((tall, PADDED - CHANNEL_PER_PART), part_w.dtype)
            wpad[t, pl.ds(r, tall), h * PADDED : (h + 1) * PADDED] = jnp.concatenate(
                [part_w, empty], axis=1
            )

    @pl.loop(2, 4)
    def _(i):
        norm(i)
        send(i)

    w_stage(1)

    @pl.loop(0, 4)
    def _(i):
        norm(i + 4)
        send(i + 4)
        forward(i)

        @pl.when(i > 0)
        def _():
            project_qkv(i - 1)

        @pl.when(i == 2)
        def _():
            w_stage(2)

    per = lanes // 4

    @pl.loop(0, 4)
    def _(i):
        forward(i + 4)
        project_qkv(i + 3)
        for n in range(per):
            attend_and_send(0, lanes - 1 - i * per - n)

    for n in range(3, len(w_stages)):
        w_stage(n)
    project_qkv(pieces - 1)

    @pl.loop(0, lanes)
    def _(i):
        attend_and_send(1, lanes - 1 - i)

    for n in range(max(3, len(w_stages)), len(w_stages) + 1):
        w_stage(n)
    own_copy.wait()
    for k in reversed(range(1, lanes)):
        attended_copy(0, k).wait_recv()
    project_out(0, list(range(lanes)), [])
    for window in range(1, window_count):
        project_out(window, [0], [1] + list(reversed(range(2, lanes))))

    for copy in fetches:
        copy.wait_send()

    @pl.loop(0, pieces)
    def _(i):
        for k in range(1, lanes):
            gather_copy(k, i).wait_send()

    for copy in w_copies:
        copy.wait_send()
    for window in range(window_count):
        for k in range(1, lanes):
            attended_copy(window, k).wait_send()
        for copy in emit(window):
            copy.wait()


def share_levels(members, blocks, head_width):
    by_member = int(members == 2 and head_width % 32 == 0)
    by_win = int(by_member and blocks % 2 == 0 and head_width % 64 == 0)
    return by_member, by_win


def on_device(x, labels, gain, offset, wqkv, scale, wout):
    lanes = lax.axis_size("seq")
    blocks = lax.axis_size("win")
    members = lax.axis_size("member")
    _, rows, _, cols, width = x.shape
    step = rows // 2
    window_count = cols // WS
    pieces = 4 * window_count
    head_width = wout.shape[0]
    heads = head_width // CHANNEL_PER_PART
    group = step * HALF
    chunk = 4 * group
    half = jnp.bfloat16
    w_count = 4 * lanes
    vmem = pl.BlockSpec(memory_space=pltpu.VMEM)
    anywhere = pl.BlockSpec(memory_space=pl.ANY)
    return pl.pallas_call(
        functools.partial(layer_kernel, lanes, blocks, members),
        out_shape=jax.ShapeDtypeStruct(x.shape, x.dtype),
        in_specs=[
            pl.BlockSpec(memory_space=pltpu.SMEM),
            anywhere,
            vmem,
            vmem,
            vmem,
            anywhere,
            anywhere,
        ],
        out_specs=anywhere,
        scratch_shapes=[
            pltpu.VMEM((pieces, step, HALF, width), half),
            pltpu.VMEM((lanes, pieces, step, HALF, width), half),
            pltpu.VMEM(wqkv.shape, half),
            pltpu.VMEM((3, width, heads * PADDED), half),
            pltpu.VMEM((lanes, head_width, width), half),
            pltpu.VMEM((3, window_count, lanes, 4, group, heads * PADDED), half),
            pltpu.VMEM((pieces, lanes, step, HALF, PADDED), half),
            pltpu.VMEM((pieces, lanes, step, HALF, PADDED), half),
            pltpu.VMEM((8, 128), jnp.float32),
            pltpu.VMEM((window_count, lanes, chunk, head_width), half),
            pltpu.VMEM((window_count, lanes, chunk, head_width), half),
            pltpu.VMEM((chunk, width), jnp.float32),
            pltpu.VMEM((pieces, step, HALF, width), half),
            pltpu.SemaphoreType.DMA((pieces,)),
            pltpu.SemaphoreType.DMA((pieces,)),
            pltpu.SemaphoreType.DMA((lanes, pieces)),
            pltpu.SemaphoreType.DMA((lanes, pieces)),
            pltpu.SemaphoreType.DMA((window_count, lanes)),
            pltpu.SemaphoreType.DMA((window_count, lanes)),
            pltpu.SemaphoreType.DMA((w_count,)),
            pltpu.SemaphoreType.DMA((w_count,)),
            pltpu.SemaphoreType.DMA((2,)),
            pltpu.SemaphoreType.DMA((pieces,)),
        ],
        compiler_params=pltpu.CompilerParams(
            collective_id=0, has_side_effects=True, vmem_limit_bytes=58 << 20
        ),
    )(scale, x, labels, gain, offset, wqkv, wout)


def solution(mesh):
    in_specs = (
        P(("member", "win"), None, "seq", None, None),
        P(("member", "win"), None, None),
        P(),
        P(),
        P(None, None, "seq"),
        P("seq"),
        P("seq", None),
    )
    out_specs = P(("member", "win"), None, "seq", None, None)
    return jax.shard_map(
        on_device, mesh=mesh, in_specs=in_specs, out_specs=out_specs, check_vma=False
    )
```

```python
import functools
import math

import jax
import jax.numpy as jnp
from jax import lax
from jax.experimental import pallas as pl
from jax.experimental.pallas import tpu as pltpu
from jax.sharding import PartitionSpec as P

CHANNEL_PER_PART = 96
PADDED = 128
WS = 32
HALF = WS // 2
LOG2E = 1.4426950408889634
MESH = pl.DeviceIdType.MESH


def xor(value, mask, bits):
    both = 0
    for b in range(bits):
        both = both + (1 << b) * ((value // (1 << b)) % 2) * ((mask // (1 << b)) % 2)
    return value + mask - 2 * both


def flip(value, bit=1):
    return value + bit - 2 * bit * ((value // bit) % 2)


def children(slot, lanes):
    low = lanes if slot == 0 else slot & -slot
    masks = [1 << b for b in reversed(range(lanes.bit_length() - 1))]
    return [slot | m for m in masks if m < low]


def layer_kernel(
    lanes,
    blocks,
    members,
    scale_hbm,
    x_ref,
    label_hbm,
    gain_hbm,
    bias_hbm,
    wqkv_ref,
    wout_ref,
    out_ref,
    scale_ref,
    label_ref,
    gain_ref,
    bias_ref,
    pix,
    nrm,
    raw,
    wpad,
    wall,
    qkv,
    extq,
    extk,
    labt,
    att_out,
    att_in,
    acc,
    fetch_send,
    fetch_recv,
    norm_send,
    norm_recv,
    att_send,
    att_recv,
    w_send,
    w_recv,
    local_sem,
):
    me = lax.axis_index("seq")
    win = lax.axis_index("win")
    member = lax.axis_index("member")
    bits = lanes.bit_length() - 1
    pieces, step, _, width = pix.shape
    rows = 2 * step
    group = step * HALF
    chunk = 4 * group
    window_count = pieces // 4
    head_width = att_out.shape[3]
    heads = head_width // CHANNEL_PER_PART
    cols = window_count * WS

    def at_seq(mask):
        return {"seq": xor(me, mask, bits)}

    def source(i):
        window, place, side = i // 4, (i // 2) % 2, i % 2
        first = window * WS + HALF + side * HALF
        span = pl.ds(step, step) if place == 0 else pl.ds(0, step)
        return place, first, x_ref.at[0, span, 0, pl.ds(first % cols, HALF), :]

    west = (win + blocks - 2) % blocks
    fetches = []
    locals_ = []
    for i in range(pieces):
        place, first, src = source(i)
        if place == 0 and first < cols:
            locals_.append(pltpu.make_async_copy(src, pix.at[i], fetch_recv.at[i]))
            continue
        if first < cols:
            to = flip(win)
        else:
            to = west if place == 0 else flip(west)
        fetches.append(
            pltpu.make_async_remote_copy(
                src_ref=src,
                dst_ref=pix.at[i],
                send_sem=fetch_send.at[i],
                recv_sem=fetch_recv.at[i],
                device_id={"win": to},
                device_id_type=MESH,
            )
        )

    def gather_copy(slot, i):
        parent = slot & (slot - 1)
        return pltpu.make_async_remote_copy(
            src_ref=nrm.at[parent, i],
            dst_ref=nrm.at[slot, i],
            send_sem=norm_send.at[slot, i],
            recv_sem=norm_recv.at[slot, i],
            device_id=at_seq(slot ^ parent),
            device_id_type=MESH,
        )

    def attended_copy(window, k):
        return pltpu.make_async_remote_copy(
            src_ref=att_out.at[window, k],
            dst_ref=att_in.at[window, k],
            send_sem=att_send.at[window, k],
            recv_sem=att_recv.at[window, k],
            device_id=at_seq(k),
            device_id_type=MESH,
        )

    w_copies = []

    def w_copy(src, dst, device):
        n = len(w_copies)
        copy = pltpu.make_async_remote_copy(
            src_ref=src,
            dst_ref=dst,
            send_sem=w_send.at[n],
            recv_sem=w_recv.at[n],
            device_id=device,
            device_id_type=MESH,
        )
        w_copies.append(copy)
        return copy

    def slot_rows(slot, start, count):
        if slot == 0:
            return wout_ref.at[pl.ds(start, count), :]
        return wall.at[slot, pl.ds(start, count), :]

    share_member, share_win = share_levels(members, blocks, head_width)
    part = head_width // (1 + share_member) // (1 + share_win)
    pair = part * (1 + share_member)
    w_stages = [[]]
    held = [0]
    masks = [1 << b for b in reversed(range(bits))]
    for mask in masks:
        grown = [k | mask for k in held]
        if mask == 1:
            direct = [w_copy(slot_rows(0, 0, head_width), wall.at[1], at_seq(1))]
            w_stages[0] += direct
            w_stages.append(
                [w_copy(wall.at[k], wall.at[k | 1], at_seq(1)) for k in held if k]
            )
        else:
            start = 0
            if share_win:
                start = (win % 2) * pair
            own = start
            if share_member:
                own = start + member * part
            own = pl.multiple_of(own, 16) if share_win or share_member else own
            stage = [
                w_copy(slot_rows(k, own, part), wall.at[k | mask, pl.ds(own, part), :], at_seq(mask))
                for k in held
            ]
            if held == [0]:
                w_stages[0] += stage
            else:
                w_stages.append(stage)
            if share_member:
                w_stages.append(
                    [
                        w_copy(
                            wall.at[k, pl.ds(own, part), :],
                            wall.at[k, pl.ds(own, part), :],
                            {"member": flip(member)},
                        )
                        for k in grown
                    ]
                )
            if share_win:
                begin = pl.multiple_of(start, 16)
                w_stages.append(
                    [
                        w_copy(
                            wall.at[k, pl.ds(begin, pair), :],
                            wall.at[k, pl.ds(begin, pair), :],
                            {"win": flip(win)},
                        )
                        for k in grown
                    ]
                )
        held = held + grown

    def w_stage(n):
        if 0 < n <= len(w_stages):
            for copy in w_stages[n - 1]:
                copy.wait_recv()
        if n < len(w_stages):
            for copy in w_stages[n]:
                copy.start()

    def norm(i):
        pltpu.make_async_copy(pix.at[i], pix.at[i], fetch_recv.at[i]).wait()
        gain = gain_ref[...]
        offset = bias_ref[...]
        for a in range(step):
            values = pix[i, a].astype(jnp.float32)
            average = jnp.mean(values, axis=-1, keepdims=True)
            centred = values - average
            variance = jnp.mean(centred * centred, axis=-1, keepdims=True)
            scaled = centred * lax.rsqrt(variance + 1e-05) * gain + offset
            nrm[0, i, a] = scaled.astype(jnp.bfloat16)

    def send(i):
        for slot in children(0, lanes):
            gather_copy(slot, i).start()

    inner = [k for k in range(1, lanes) if children(k, lanes)]
    inner.sort(key=lambda k: (bin(k).count("1"), -k))

    def forward(i):
        for k in inner:
            gather_copy(k, i).wait_recv()
            for slot in children(k, lanes):
                gather_copy(slot, i).start()

    def project_qkv(i):
        for k in range(1, lanes):
            if not children(k, lanes):
                gather_copy(k, i).wait_recv()
        window, place = i // 4, i % 4
        x = nrm[:, i].reshape(lanes * group, width)
        lane = lax.broadcasted_iota(jnp.int32, (lanes * group, PADDED), 1)
        ones = jnp.where(lane == CHANNEL_PER_PART, 1.0, 0.0).astype(jnp.bfloat16)
        q_extra = extq[i].reshape(lanes * group, PADDED)
        k_extra = extk[i].reshape(lanes * group, PADDED)
        for t, extra in enumerate((q_extra, k_extra, ones)):
            y = jnp.dot(x, wpad[t], preferred_element_type=jnp.float32).astype(jnp.bfloat16)
            for h in range(heads):
                part_y = y[:, h * PADDED : (h + 1) * PADDED] + extra
                qkv[t, window, :, place, :, h * PADDED : (h + 1) * PADDED] = part_y.reshape(
                    lanes, group, PADDED
                )

    def attend(window, k):
        for h in range(heads):
            span = slice(h * PADDED, (h + 1) * PADDED)
            tempered = scale_ref[h : h + 1].reshape(1, 1) * (LOG2E / math.sqrt(CHANNEL_PER_PART))
            q = qkv[0, window, k, :, :, span].reshape(chunk, PADDED)
            keys = qkv[1, window, :, :, :, span].reshape(lanes * chunk, PADDED)
            values = qkv[2, window, :, :, :, span].reshape(lanes * chunk, PADDED)
            scores = lax.dot_general(
                q, keys, (((1,), (1,)), ((), ())), preferred_element_type=jnp.float32
            )
            row_max = jnp.max(scores, axis=-1, keepdims=True)
            numerators = jnp.exp2((scores - row_max) * tempered).astype(jnp.bfloat16)
            summed = jnp.dot(numerators, values, preferred_element_type=jnp.float32)
            attended = summed / summed[:, CHANNEL_PER_PART : CHANNEL_PER_PART + 1]
            att_out[window, k, :, h * CHANNEL_PER_PART : (h + 1) * CHANNEL_PER_PART] = attended[
                :, :CHANNEL_PER_PART
            ].astype(jnp.bfloat16)

    def attend_and_send(window, k):
        attend(window, k)

        @pl.when(k > 0)
        def _():
            attended_copy(window, k).start()

    tile = 512 if width % 512 == 0 else width

    def store(window, columns, total):
        total = total.astype(jnp.bfloat16).reshape(4, step, HALF, tile)
        for piece in range(4):
            first = window * WS + (piece % 2) * HALF
            start = (piece // 2) * step
            out_ref[0, start : start + step, 0, first : first + HALF, columns] = total[piece]

    def residual(window, columns):
        return pix[window * 4 : window * 4 + 4, :, :, columns].reshape(chunk, tile).astype(jnp.float32)

    def project_out(window, ready, late):
        for start in range(0, width, tile):
            columns = slice(start, start + tile)
            total = residual(window, columns)
            for k in ready:
                source_ref = att_out if k == 0 else att_in
                total += jnp.dot(
                    source_ref[window, k], wall[k, :, columns], preferred_element_type=jnp.float32
                )
            if late:
                acc[:, columns] = total
            else:
                store(window, columns, total)
        for n, k in enumerate(late):
            attended_copy(window, k).wait_recv()
            for start in range(0, width, tile):
                columns = slice(start, start + tile)
                total = acc[:, columns] + jnp.dot(
                    att_in[window, k], wall[k, :, columns], preferred_element_type=jnp.float32
                )
                if n + 1 < len(late):
                    acc[:, columns] = total
                else:
                    store(window, columns, total)

    barrier = pltpu.get_barrier_semaphore()
    greeted = [at_seq(k) for k in range(1, lanes)]
    greeted += [{"win": flip(win)}, {"win": (win + 2) % blocks}, {"win": (flip(win) + 2) % blocks}]
    if share_member:
        greeted.append({"member": flip(member)})
    for device in greeted:
        pl.semaphore_signal(barrier, inc=1, device_id=device, device_id_type=MESH)
    for copy in locals_:
        copy.start()
    loads = [
        pltpu.make_async_copy(src, dst, local_sem.at[n])
        for n, (src, dst) in enumerate(
            [
                (gain_hbm, gain_ref),
                (bias_hbm, bias_ref),
                (label_hbm, label_ref),
                (scale_hbm, scale_ref),
                (wqkv_ref, raw),
                (wout_ref, wall.at[0]),
            ]
        )
    ]
    for copy in loads:
        copy.start()
    pl.semaphore_wait(barrier, len(greeted))
    for copy in fetches:
        copy.start()
    w_stage(0)
    loads[0].wait()
    loads[1].wait()

    @pl.loop(0, 2)
    def _(i):
        norm(i)
        send(i)

    labt[...] = jnp.zeros_like(labt)
    loads[2].wait()
    for k in range(lanes):
        lane_of = xor(me, k, bits)
        for a in range(rows):
            labt[a : a + 1, :cols] = label_ref[0, pl.ds(a * lanes + lane_of, 1), :].astype(jnp.float32)
        turned = jnp.transpose(labt[...])
        for i in range(pieces):
            first = (i // 4) * WS + (i % 2) * HALF
            for a in range(step):
                row = ((i // 2) % 2) * step + a
                label = turned[first : first + HALF, row : row + 1].astype(jnp.int32)
                lane = lax.broadcasted_iota(jnp.int32, (HALF, PADDED), 1) - CHANNEL_PER_PART
                same = lane == label
                extq[i, k, a] = jnp.where(same, 1.0, 0.0).astype(jnp.bfloat16)
                extk[i, k, a] = jnp.where(
                    jnp.logical_and(lane >= 0, jnp.logical_not(same)), -1e30, 0.0
                ).astype(jnp.bfloat16)

    loads[3].wait()
    loads[4].wait()
    tall = width // 4

    @pl.loop(0, 12)
    def _(n):
        t, r = n // 4, pl.multiple_of((n % 4) * tall, tall)
        for h in range(heads):
            part_w = raw[t, pl.ds(r, tall), h * CHANNEL_PER_PART : (h + 1) * CHANNEL_PER_PART]
            empty = jnp.zeros((tall, PADDED - CHANNEL_PER_PART), part_w.dtype)
            wpad[t, pl.ds(r, tall), h * PADDED : (h + 1) * PADDED] = jnp.concatenate(
                [part_w, empty], axis=1
            )

    @pl.loop(2, 4)
    def _(i):
        norm(i)
        send(i)

    w_stage(1)

    @pl.loop(0, 4)
    def _(i):
        norm(i + 4)
        send(i + 4)
        forward(i)

        @pl.when(i > 0)
        def _():
            project_qkv(i - 1)

        @pl.when(i == 2)
        def _():
            w_stage(2)

    per = lanes // 4

    @pl.loop(0, 4)
    def _(i):
        forward(i + 4)
        project_qkv(i + 3)
        for n in range(per):
            attend_and_send(0, lanes - 1 - i * per - n)

    for n in range(3, len(w_stages)):
        w_stage(n)
    project_qkv(pieces - 1)

    @pl.loop(0, lanes)
    def _(i):
        attend_and_send(1, lanes - 1 - i)

    for n in range(max(3, len(w_stages)), len(w_stages) + 1):
        w_stage(n)
    loads[5].wait()
    for k in reversed(range(1, lanes)):
        attended_copy(0, k).wait_recv()
    project_out(0, list(range(lanes)), [])
    for window in range(1, window_count):
        project_out(window, [0], [1] + list(reversed(range(2, lanes))))

    for copy in fetches:
        copy.wait_send()

    @pl.loop(0, pieces)
    def _(i):
        for k in range(1, lanes):
            gather_copy(k, i).wait_send()

    for copy in w_copies:
        copy.wait_send()
    for window in range(window_count):
        for k in range(1, lanes):
            attended_copy(window, k).wait_send()


def share_levels(members, blocks, head_width):
    by_member = int(members == 2 and head_width % 32 == 0)
    by_win = int(by_member and blocks % 2 == 0 and head_width % 64 == 0)
    return by_member, by_win


def on_device(x, labels, gain, offset, wqkv, scale, wout):
    lanes = lax.axis_size("seq")
    blocks = lax.axis_size("win")
    members = lax.axis_size("member")
    _, rows, _, cols, width = x.shape
    step = rows // 2
    window_count = cols // WS
    pieces = 4 * window_count
    head_width = wout.shape[0]
    heads = head_width // CHANNEL_PER_PART
    group = step * HALF
    chunk = 4 * group
    half = jnp.bfloat16
    w_count = 4 * lanes
    in_hbm = functools.partial(pltpu.with_memory_space_constraint, memory_space=pltpu.HBM)
    operands = (scale, x, labels, gain, offset, wqkv, wout)
    return pl.pallas_call(
        functools.partial(layer_kernel, lanes, blocks, members),
        out_shape=pltpu.VMEM(x.shape, x.dtype),
        in_specs=[pl.BlockSpec(memory_space=pltpu.HBM)] * 7,
        out_specs=pl.BlockSpec(memory_space=pltpu.VMEM),
        scratch_shapes=[
            pltpu.VMEM(scale.shape, scale.dtype),
            pltpu.VMEM(labels.shape, labels.dtype),
            pltpu.VMEM(gain.shape, gain.dtype),
            pltpu.VMEM(offset.shape, offset.dtype),
            pltpu.VMEM((pieces, step, HALF, width), half),
            pltpu.VMEM((lanes, pieces, step, HALF, width), half),
            pltpu.VMEM(wqkv.shape, half),
            pltpu.VMEM((3, width, heads * PADDED), half),
            pltpu.VMEM((lanes, head_width, width), half),
            pltpu.VMEM((3, window_count, lanes, 4, group, heads * PADDED), half),
            pltpu.VMEM((pieces, lanes, step, HALF, PADDED), half),
            pltpu.VMEM((pieces, lanes, step, HALF, PADDED), half),
            pltpu.VMEM((8, 128), jnp.float32),
            pltpu.VMEM((window_count, lanes, chunk, head_width), half),
            pltpu.VMEM((window_count, lanes, chunk, head_width), half),
            pltpu.VMEM((chunk, width), jnp.float32),
            pltpu.SemaphoreType.DMA((pieces,)),
            pltpu.SemaphoreType.DMA((pieces,)),
            pltpu.SemaphoreType.DMA((lanes, pieces)),
            pltpu.SemaphoreType.DMA((lanes, pieces)),
            pltpu.SemaphoreType.DMA((window_count, lanes)),
            pltpu.SemaphoreType.DMA((window_count, lanes)),
            pltpu.SemaphoreType.DMA((w_count,)),
            pltpu.SemaphoreType.DMA((w_count,)),
            pltpu.SemaphoreType.DMA((6,)),
        ],
        compiler_params=pltpu.CompilerParams(
            collective_id=0, has_side_effects=True, vmem_limit_bytes=42 << 20
        ),
    )(*[in_hbm(o) if o.size > 1 else o for o in operands])


def solution(mesh):
    in_specs = (
        P(("member", "win"), None, "seq", None, None),
        P(("member", "win"), None, None),
        P(),
        P(),
        P(None, None, "seq"),
        P("seq"),
        P("seq", None),
    )
    out_specs = P(("member", "win"), None, "seq", None, None)
    return jax.shard_map(
        on_device, mesh=mesh, in_specs=in_specs, out_specs=out_specs, check_vma=False
    )
```

```python
import functools
import math

import jax
import jax.numpy as jnp
from jax import lax
from jax.experimental import pallas as pl
from jax.experimental.pallas import tpu as pltpu
from jax.sharding import PartitionSpec as P

CHANNEL_PER_PART = 96
PADDED = 128
WS = 32
HALF = WS // 2
LOG2E = 1.4426950408889634
MESH = pl.DeviceIdType.MESH


def xor(value, mask, bits):
    both = 0
    for b in range(bits):
        both = both + (1 << b) * ((value // (1 << b)) % 2) * ((mask // (1 << b)) % 2)
    return value + mask - 2 * both


def flip(value, bit=1):
    return value + bit - 2 * bit * ((value // bit) % 2)


def children(slot, lanes):
    low = lanes if slot == 0 else slot & -slot
    masks = [1 << b for b in reversed(range(lanes.bit_length() - 1))]
    return [slot | m for m in masks if m < low]


def layer_kernel(
    lanes,
    blocks,
    members,
    scale_hbm,
    x_ref,
    label_hbm,
    gain_hbm,
    bias_hbm,
    wqkv_ref,
    wout_ref,
    out_ref,
    scale_ref,
    label_ref,
    gain_ref,
    bias_ref,
    pix,
    nrm,
    raw,
    wpad,
    wall,
    qkv,
    extq,
    extk,
    labt,
    att_out,
    att_in,
    acc,
    fetch_send,
    fetch_recv,
    norm_send,
    norm_recv,
    att_send,
    att_recv,
    w_send,
    w_recv,
    local_sem,
    known_sem,
):
    me = lax.axis_index("seq")
    win = lax.axis_index("win")
    member = lax.axis_index("member")
    bits = lanes.bit_length() - 1
    pieces, step, _, width = pix.shape
    rows = 2 * step
    group = step * HALF
    chunk = 4 * group
    window_count = pieces // 4
    head_width = att_out.shape[3]
    heads = head_width // CHANNEL_PER_PART
    cols = window_count * WS

    def at_seq(mask):
        return {"seq": xor(me, mask, bits)}

    def source(i):
        window, place, side = i // 4, (i // 2) % 2, i % 2
        first = window * WS + HALF + side * HALF
        span = pl.ds(step, step) if place == 0 else pl.ds(0, step)
        return place, first, x_ref.at[0, span, 0, pl.ds(first % cols, HALF), :]

    west = (win + blocks - 2) % blocks
    fetches = []
    corners = []
    locals_ = []

    def fetch_copy(src, dst, n, to):
        return pltpu.make_async_remote_copy(
            src_ref=src,
            dst_ref=dst,
            send_sem=fetch_send.at[n],
            recv_sem=fetch_recv.at[n],
            device_id={"win": to},
            device_id_type=MESH,
        )

    for i in range(pieces):
        place, first, src = source(i)
        if place == 0 and first < cols:
            locals_.append(pltpu.make_async_copy(src, pix.at[i], fetch_recv.at[i]))
            continue
        if place == 1 and first >= cols:
            corners.append(fetch_copy(src, pix.at[i], i, flip(west)))
        else:
            fetches.append(fetch_copy(src, pix.at[i], i, flip(win) if place else west))

    def gather_copy(slot, i):
        parent = slot & (slot - 1)
        return pltpu.make_async_remote_copy(
            src_ref=nrm.at[parent, i],
            dst_ref=nrm.at[slot, i],
            send_sem=norm_send.at[slot, i],
            recv_sem=norm_recv.at[slot, i],
            device_id=at_seq(slot ^ parent),
            device_id_type=MESH,
        )

    def attended_copy(window, k):
        return pltpu.make_async_remote_copy(
            src_ref=att_out.at[window, k],
            dst_ref=att_in.at[window, k],
            send_sem=att_send.at[window, k],
            recv_sem=att_recv.at[window, k],
            device_id=at_seq(k),
            device_id_type=MESH,
        )

    w_copies = []

    def w_copy(src, dst, device):
        n = len(w_copies)
        copy = pltpu.make_async_remote_copy(
            src_ref=src,
            dst_ref=dst,
            send_sem=w_send.at[n],
            recv_sem=w_recv.at[n],
            device_id=device,
            device_id_type=MESH,
        )
        w_copies.append(copy)
        return copy

    def slot_rows(slot, start, count):
        if slot == 0:
            return wout_ref.at[pl.ds(start, count), :]
        return wall.at[slot, pl.ds(start, count), :]

    share_member, share_win, share_far = share_levels(members, blocks, head_width)
    part = head_width // (1 + share_member) // (1 + share_win) // (1 + share_far)
    near, far = (win % 2) * share_win, ((win // 2) % 2) * share_far
    mine = member * share_member

    def rows_of(b, a, m, count=1):
        start = (((b * (1 + share_far)) + a) * (1 + share_member) + m) * part
        if not isinstance(start, int):
            start = pl.multiple_of(start, 16)
        return start, count * part

    def relay(slots, place, device):
        return [
            w_copy(wall.at[k, pl.ds(*place), :], wall.at[k, pl.ds(*place), :], device)
            for k in slots
        ]

    w_stages = []
    held = [0]
    pending = []
    for mask in [1 << b for b in reversed(range(bits))]:
        grown = [k | mask for k in held]
        if mask == 1:
            direct = [w_copy(slot_rows(0, 0, head_width), wall.at[1], at_seq(1))]
            last = [w_copy(wall.at[k], wall.at[k | 1], at_seq(1)) for k in held if k]
            if w_stages:
                w_stages[0] = (w_stages[0][0], w_stages[0][1] + direct)
                w_stages.append((pending, last))
            else:
                w_stages.append(([], direct))
            pending = last + direct
        else:
            place = rows_of(near, far, mine)
            stage = [
                w_copy(slot_rows(k, *place), wall.at[k | mask, pl.ds(*place), :], at_seq(mask))
                for k in held
            ]
            w_stages.append((pending, stage))
            pending = stage
            if share_far:
                other = 1 - far
                up = relay(grown, place, {"member": flip(member)})
                over = relay(grown, place, {"win": flip(win, 2)})
                w_stages.append((pending, up + over))
                across = relay(grown, rows_of(near, other, mine), {"member": flip(member)})
                batch = relay(grown, rows_of(near, far, 0, 2), {"win": flip(win)})
                batch += relay(grown, rows_of(near, other, mine), {"win": flip(win)})
                w_stages.append((up + over, across + batch))
                rest = relay(grown, rows_of(near, other, 1 - mine), {"win": flip(win)})
                w_stages.append((across, rest))
                pending = batch + rest
            else:
                if share_member:
                    stage = relay(grown, place, {"member": flip(member)})
                    w_stages.append((pending, stage))
                    pending = stage
                if share_win:
                    stage = relay(grown, rows_of(near, 0, 0, 1 + share_member), {"win": flip(win)})
                    w_stages.append((pending, stage))
                    pending = stage
        held = held + grown
    w_stages.append((pending, []))

    def w_stage(n):
        if n < len(w_stages):
            for copy in w_stages[n][0]:
                copy.wait_recv()
            for copy in w_stages[n][1]:
                copy.start()

    def norm(i):
        pltpu.make_async_copy(pix.at[i], pix.at[i], fetch_recv.at[i]).wait()
        gain = gain_ref[...]
        offset = bias_ref[...]
        for a in range(step):
            values = pix[i, a].astype(jnp.float32)
            average = jnp.mean(values, axis=-1, keepdims=True)
            centred = values - average
            variance = jnp.mean(centred * centred, axis=-1, keepdims=True)
            scaled = centred * lax.rsqrt(variance + 1e-05) * gain + offset
            nrm[0, i, a] = scaled.astype(jnp.bfloat16)

    def send(i):
        for slot in children(0, lanes):
            gather_copy(slot, i).start()

    inner = [k for k in range(1, lanes) if children(k, lanes)]
    inner.sort(key=lambda k: (bin(k).count("1"), -k))

    def forward(i):
        for k in inner:
            gather_copy(k, i).wait_recv()
            for slot in children(k, lanes):
                gather_copy(slot, i).start()

    def project_qkv(i):
        for k in range(1, lanes):
            if not children(k, lanes):
                gather_copy(k, i).wait_recv()
        window, place = i // 4, i % 4
        x = nrm[:, i].reshape(lanes * group, width)
        lane = lax.broadcasted_iota(jnp.int32, (lanes * group, PADDED), 1)
        ones = jnp.where(lane == CHANNEL_PER_PART, 1.0, 0.0).astype(jnp.bfloat16)
        q_extra = extq[i].reshape(lanes * group, PADDED)
        k_extra = extk[i].reshape(lanes * group, PADDED)
        for t, extra in enumerate((q_extra, k_extra, ones)):
            y = jnp.dot(x, wpad[t], preferred_element_type=jnp.float32).astype(jnp.bfloat16)
            for h in range(heads):
                part_y = y[:, h * PADDED : (h + 1) * PADDED] + extra
                qkv[t, window, :, place, :, h * PADDED : (h + 1) * PADDED] = part_y.reshape(
                    lanes, group, PADDED
                )

    def scores_of(window, k, h):
        span = slice(h * PADDED, (h + 1) * PADDED)
        q = qkv[0, window, k, :, :, span].reshape(chunk, PADDED)
        keys = qkv[1, window, :, :, :, span].reshape(lanes * chunk, PADDED)
        return lax.dot_general(
            q, keys, (((1,), (1,)), ((), ())), preferred_element_type=jnp.float32
        )

    def attend(window, k):
        scores = scores_of(window, k, 0)
        for h in range(heads):
            following = scores_of(window, k, h + 1) if h + 1 < heads else None
            tempered = scale_ref[h : h + 1].reshape(1, 1) * (LOG2E / math.sqrt(CHANNEL_PER_PART))
            values = qkv[2, window, :, :, :, h * PADDED : (h + 1) * PADDED].reshape(
                lanes * chunk, PADDED
            )
            row_max = jnp.max(scores, axis=-1, keepdims=True)
            numerators = jnp.exp2((scores - row_max) * tempered).astype(jnp.bfloat16)
            summed = jnp.dot(numerators, values, preferred_element_type=jnp.float32)
            attended = summed / summed[:, CHANNEL_PER_PART : CHANNEL_PER_PART + 1]
            att_out[window, k, :, h * CHANNEL_PER_PART : (h + 1) * CHANNEL_PER_PART] = attended[
                :, :CHANNEL_PER_PART
            ].astype(jnp.bfloat16)
            scores = following

    def attend_and_send(window, k):
        attend(window, k)

        @pl.when(k > 0)
        def _():
            attended_copy(window, k).start()

    tile = 512 if width % 512 == 0 else width

    def store(window, columns, total):
        total = total.astype(jnp.bfloat16).reshape(4, step, HALF, tile)
        for piece in range(4):
            first = window * WS + (piece % 2) * HALF
            start = (piece // 2) * step
            out_ref[0, start : start + step, 0, first : first + HALF, columns] = total[piece]

    def residual(window, columns):
        return pix[window * 4 : window * 4 + 4, :, :, columns].reshape(chunk, tile).astype(jnp.float32)

    def project_out(window, ready, late):
        for start in range(0, width, tile):
            columns = slice(start, start + tile)
            total = residual(window, columns)
            for k in ready:
                source_ref = att_out if k == 0 else att_in
                total += jnp.dot(
                    source_ref[window, k], wall[k, :, columns], preferred_element_type=jnp.float32
                )
            if late:
                acc[:, columns] = total
            else:
                store(window, columns, total)
        for n, k in enumerate(late):
            attended_copy(window, k).wait_recv()
            for start in range(0, width, tile):
                columns = slice(start, start + tile)
                total = acc[:, columns] + jnp.dot(
                    att_in[window, k], wall[k, :, columns], preferred_element_type=jnp.float32
                )
                if n + 1 < len(late):
                    acc[:, columns] = total
                else:
                    store(window, columns, total)

    barrier = pltpu.get_barrier_semaphore()
    greeted = [at_seq(k) for k in range(1, lanes)]
    greeted += [{"win": flip(win)}, {"win": (win + 2) % blocks}]
    if share_far and blocks != 4:
        greeted.append({"win": flip(win, 2)})
    if share_member:
        greeted.append({"member": flip(member)})
    for device in greeted:
        pl.semaphore_signal(barrier, inc=1, device_id=device, device_id_type=MESH)
    for copy in locals_:
        copy.start()
    loads = [
        pltpu.make_async_copy(src, dst, local_sem.at[n])
        for n, (src, dst) in enumerate(
            [
                (gain_hbm, gain_ref),
                (bias_hbm, bias_ref),
                (label_hbm, label_ref),
                (scale_hbm, scale_ref),
                (wqkv_ref, raw),
                (wout_ref, wall.at[0]),
            ]
        )
    ]
    for copy in loads:
        copy.start()
    pl.semaphore_wait(barrier, len(greeted))
    pl.semaphore_signal(
        known_sem, inc=1, device_id={"win": (win + 2) % blocks}, device_id_type=MESH
    )
    for copy in fetches:
        copy.start()
    w_stage(0)
    loads[0].wait()
    loads[1].wait()

    @pl.loop(0, 2)
    def _(i):
        norm(i)
        send(i)

    pl.semaphore_wait(known_sem, 1)
    for copy in corners:
        copy.start()

    labt[...] = jnp.zeros_like(labt)
    loads[2].wait()
    for k in range(lanes):
        lane_of = xor(me, k, bits)
        for a in range(rows):
            labt[a : a + 1, :cols] = label_ref[0, pl.ds(a * lanes + lane_of, 1), :].astype(jnp.float32)
        turned = jnp.transpose(labt[...])
        for i in range(pieces):
            first = (i // 4) * WS + (i % 2) * HALF
            for a in range(step):
                row = ((i // 2) % 2) * step + a
                label = turned[first : first + HALF, row : row + 1].astype(jnp.int32)
                lane = lax.broadcasted_iota(jnp.int32, (HALF, PADDED), 1) - CHANNEL_PER_PART
                same = lane == label
                extq[i, k, a] = jnp.where(same, 1.0, 0.0).astype(jnp.bfloat16)
                extk[i, k, a] = jnp.where(
                    jnp.logical_and(lane >= 0, jnp.logical_not(same)), -1e30, 0.0
                ).astype(jnp.bfloat16)

    loads[3].wait()
    loads[4].wait()
    tall = width // 4

    @pl.loop(0, 12)
    def _(n):
        t, r = n // 4, pl.multiple_of((n % 4) * tall, tall)
        for h in range(heads):
            part_w = raw[t, pl.ds(r, tall), h * CHANNEL_PER_PART : (h + 1) * CHANNEL_PER_PART]
            empty = jnp.zeros((tall, PADDED - CHANNEL_PER_PART), part_w.dtype)
            wpad[t, pl.ds(r, tall), h * PADDED : (h + 1) * PADDED] = jnp.concatenate(
                [part_w, empty], axis=1
            )

    @pl.loop(2, 4)
    def _(i):
        norm(i)
        send(i)

    w_stage(1)

    @pl.loop(0, 4)
    def _(i):
        norm(i + 4)
        send(i + 4)
        forward(i)

        @pl.when(i > 0)
        def _():
            project_qkv(i - 1)

    per = lanes // 4

    @pl.loop(0, 4)
    def _(i):
        forward(i + 4)
        project_qkv(i + 3)

        @pl.when(i == 0)
        def _():
            w_stage(2)

        @pl.when(i == 2)
        def _():
            w_stage(3)

        @pl.when(i < 3)
        def _():
            for n in range(per):
                attend_and_send(0, lanes - 1 - i * per - n)

    project_qkv(pieces - 1)

    @pl.loop(0, 2 * per)
    def _(i):
        attend_and_send(1, lanes - 1 - i)

    for n in range(4, len(w_stages) - 1):
        w_stage(n)

    @pl.loop(0, 3 * per)
    def _(i):
        window = (i + 2 * per) // (3 * per)
        attend_and_send(window, per - 1 - i + 2 * per * window)

    w_stage(max(4, len(w_stages) - 1))
    loads[5].wait()
    for k in reversed(range(1, lanes)):
        attended_copy(0, k).wait_recv()
    project_out(0, list(range(lanes)), [])
    for window in range(1, window_count):
        project_out(window, [0], [1] + list(reversed(range(2, lanes))))

    for copy in fetches + corners:
        copy.wait_send()

    @pl.loop(0, pieces)
    def _(i):
        for k in range(1, lanes):
            gather_copy(k, i).wait_send()

    for copy in w_copies:
        copy.wait_send()
    for window in range(window_count):
        for k in range(1, lanes):
            attended_copy(window, k).wait_send()


def share_levels(members, blocks, head_width):
    by_member = int(members == 2 and head_width % 32 == 0)
    by_win = int(by_member and blocks % 2 == 0 and head_width % 64 == 0)
    by_far = int(by_win and blocks % 4 == 0 and head_width % 128 == 0)
    return by_member, by_win, by_far


def on_device(x, labels, gain, offset, wqkv, scale, wout):
    lanes = lax.axis_size("seq")
    blocks = lax.axis_size("win")
    members = lax.axis_size("member")
    _, rows, _, cols, width = x.shape
    step = rows // 2
    window_count = cols // WS
    pieces = 4 * window_count
    head_width = wout.shape[0]
    heads = head_width // CHANNEL_PER_PART
    group = step * HALF
    chunk = 4 * group
    half = jnp.bfloat16
    w_count = 4 * lanes
    in_hbm = functools.partial(pltpu.with_memory_space_constraint, memory_space=pltpu.HBM)
    operands = (scale, x, labels, gain, offset, wqkv, wout)
    return pl.pallas_call(
        functools.partial(layer_kernel, lanes, blocks, members),
        out_shape=pltpu.VMEM(x.shape, x.dtype),
        in_specs=[pl.BlockSpec(memory_space=pltpu.HBM)] * 7,
        out_specs=pl.BlockSpec(memory_space=pltpu.VMEM),
        scratch_shapes=[
            pltpu.VMEM(scale.shape, scale.dtype),
            pltpu.VMEM(labels.shape, labels.dtype),
            pltpu.VMEM(gain.shape, gain.dtype),
            pltpu.VMEM(offset.shape, offset.dtype),
            pltpu.VMEM((pieces, step, HALF, width), half),
            pltpu.VMEM((lanes, pieces, step, HALF, width), half),
            pltpu.VMEM(wqkv.shape, half),
            pltpu.VMEM((3, width, heads * PADDED), half),
            pltpu.VMEM((lanes, head_width, width), half),
            pltpu.VMEM((3, window_count, lanes, 4, group, heads * PADDED), half),
            pltpu.VMEM((pieces, lanes, step, HALF, PADDED), half),
            pltpu.VMEM((pieces, lanes, step, HALF, PADDED), half),
            pltpu.VMEM((8, 128), jnp.float32),
            pltpu.VMEM((window_count, lanes, chunk, head_width), half),
            pltpu.VMEM((window_count, lanes, chunk, head_width), half),
            pltpu.VMEM((chunk, width), jnp.float32),
            pltpu.SemaphoreType.DMA((pieces,)),
            pltpu.SemaphoreType.DMA((pieces,)),
            pltpu.SemaphoreType.DMA((lanes, pieces)),
            pltpu.SemaphoreType.DMA((lanes, pieces)),
            pltpu.SemaphoreType.DMA((window_count, lanes)),
            pltpu.SemaphoreType.DMA((window_count, lanes)),
            pltpu.SemaphoreType.DMA((w_count,)),
            pltpu.SemaphoreType.DMA((w_count,)),
            pltpu.SemaphoreType.DMA((6,)),
            pltpu.SemaphoreType.REGULAR,
        ],
        compiler_params=pltpu.CompilerParams(
            collective_id=0, has_side_effects=True, vmem_limit_bytes=42 << 20
        ),
    )(*[in_hbm(o) if o.size > 1 else o for o in operands])


def solution(mesh):
    in_specs = (
        P(("member", "win"), None, "seq", None, None),
        P(("member", "win"), None, None),
        P(),
        P(),
        P(None, None, "seq"),
        P("seq"),
        P("seq", None),
    )
    out_specs = P(("member", "win"), None, "seq", None, None)
    return jax.shard_map(
        on_device, mesh=mesh, in_specs=in_specs, out_specs=out_specs, check_vma=False
    )
```

```python
import functools
import math

import jax
import jax.numpy as jnp
from jax import lax
from jax.experimental import pallas as pl
from jax.experimental.pallas import tpu as pltpu
from jax.sharding import PartitionSpec as P

CHANNEL_PER_PART = 96
PADDED = 128
WS = 32
HALF = WS // 2
LOG2E = 1.4426950408889634
MESH = pl.DeviceIdType.MESH


def xor(value, mask, bits):
    both = 0
    for b in range(bits):
        both = both + (1 << b) * ((value // (1 << b)) % 2) * ((mask // (1 << b)) % 2)
    return value + mask - 2 * both


def flip(value, bit=1):
    return value + bit - 2 * bit * ((value // bit) % 2)


def children(slot, lanes):
    low = lanes if slot == 0 else slot & -slot
    masks = [1 << b for b in reversed(range(lanes.bit_length() - 1))]
    return [slot | m for m in masks if m < low]


def layer_kernel(
    lanes,
    blocks,
    members,
    scale_hbm,
    x_ref,
    label_hbm,
    gain_hbm,
    bias_hbm,
    wqkv_ref,
    wout_ref,
    out_ref,
    scale_ref,
    label_ref,
    gain_ref,
    bias_ref,
    pix,
    nrm,
    raw,
    wpad,
    wall,
    qkv,
    extq,
    extk,
    labt,
    att_out,
    att_in,
    acc,
    fetch_send,
    fetch_recv,
    norm_send,
    norm_recv,
    att_send,
    att_recv,
    w_send,
    w_recv,
    local_sem,
    known_sem,
    near_sem,
):
    me = lax.axis_index("seq")
    win = lax.axis_index("win")
    member = lax.axis_index("member")
    bits = lanes.bit_length() - 1
    pieces, step, _, width = pix.shape
    rows = 2 * step
    group = step * HALF
    chunk = 4 * group
    window_count = pieces // 4
    head_width = att_out.shape[3]
    heads = head_width // CHANNEL_PER_PART
    cols = window_count * WS

    def at_seq(mask):
        return {"seq": xor(me, mask, bits)}

    def source(i):
        window, place, side = i // 4, (i // 2) % 2, i % 2
        first = window * WS + HALF + side * HALF
        span = pl.ds(step, step) if place == 0 else pl.ds(0, step)
        return place, first, x_ref.at[0, span, 0, pl.ds(first % cols, HALF), :]

    west = (win + blocks - 2) % blocks
    fetches = []
    corners = []
    locals_ = []

    def fetch_copy(src, dst, n, to):
        return pltpu.make_async_remote_copy(
            src_ref=src,
            dst_ref=dst,
            send_sem=fetch_send.at[n],
            recv_sem=fetch_recv.at[n],
            device_id={"win": to},
            device_id_type=MESH,
        )

    for i in range(pieces):
        place, first, src = source(i)
        if place == 0 and first < cols:
            locals_.append(pltpu.make_async_copy(src, pix.at[i], fetch_recv.at[i]))
            continue
        if place == 1 and first >= cols:
            corners.append(fetch_copy(src, pix.at[i], i, flip(west)))
        else:
            fetches.append(fetch_copy(src, pix.at[i], i, flip(win) if place else west))

    def gather_copy(slot, i):
        parent = slot & (slot - 1)
        return pltpu.make_async_remote_copy(
            src_ref=nrm.at[parent, i],
            dst_ref=nrm.at[slot, i],
            send_sem=norm_send.at[slot, i],
            recv_sem=norm_recv.at[slot, i],
            device_id=at_seq(slot ^ parent),
            device_id_type=MESH,
        )

    def attended_copy(window, k):
        return pltpu.make_async_remote_copy(
            src_ref=att_out.at[window, k],
            dst_ref=att_in.at[window, k],
            send_sem=att_send.at[window, k],
            recv_sem=att_recv.at[window, k],
            device_id=at_seq(k),
            device_id_type=MESH,
        )

    w_copies = []

    def w_copy(src, dst, device):
        n = len(w_copies)
        copy = pltpu.make_async_remote_copy(
            src_ref=src,
            dst_ref=dst,
            send_sem=w_send.at[n],
            recv_sem=w_recv.at[n],
            device_id=device,
            device_id_type=MESH,
        )
        w_copies.append(copy)
        return copy

    def slot_rows(slot, start, count):
        if slot == 0:
            return wout_ref.at[pl.ds(start, count), :]
        return wall.at[slot, pl.ds(start, count), :]

    share_member, share_win, share_far = share_levels(members, blocks, head_width)
    part = head_width // (1 + share_member) // (1 + share_win) // (1 + share_far)
    near, far = (win % 2) * share_win, ((win // 2) % 2) * share_far
    mine = member * share_member

    def rows_of(b, a, m, count=1):
        start = (((b * (1 + share_far)) + a) * (1 + share_member) + m) * part
        if not isinstance(start, int):
            start = pl.multiple_of(start, 16)
        return start, count * part

    def relay(slots, place, device):
        return [
            w_copy(wall.at[k, pl.ds(*place), :], wall.at[k, pl.ds(*place), :], device)
            for k in slots
        ]

    w_stages = []
    held = [0]
    pending = []
    for mask in [1 << b for b in reversed(range(bits))]:
        grown = [k | mask for k in held]
        if mask == 1:
            direct = [w_copy(slot_rows(0, 0, head_width), wall.at[1], at_seq(1))]
            last = [w_copy(wall.at[k], wall.at[k | 1], at_seq(1)) for k in held if k]
            if w_stages:
                w_stages[0] = (w_stages[0][0], w_stages[0][1] + direct)
                w_stages.append((pending, last))
            else:
                w_stages.append(([], direct))
            pending = last + direct
        else:
            place = rows_of(near, far, mine)
            stage = [
                w_copy(slot_rows(k, *place), wall.at[k | mask, pl.ds(*place), :], at_seq(mask))
                for k in held
            ]
            w_stages.append((pending, stage))
            pending = stage
            if share_far:
                other = 1 - far
                up = relay(grown, place, {"member": flip(member)})
                over = relay(grown, place, {"win": flip(win, 2)})
                w_stages.append((pending, up + over))
                across = relay(grown, rows_of(near, other, mine), {"member": flip(member)})
                batch = relay(grown, rows_of(near, far, 0, 2), {"win": flip(win)})
                batch += relay(grown, rows_of(near, other, mine), {"win": flip(win)})
                w_stages.append((up + over, across + batch))
                rest = relay(grown, rows_of(near, other, 1 - mine), {"win": flip(win)})
                w_stages.append((across, rest))
                pending = batch + rest
            else:
                if share_member:
                    stage = relay(grown, place, {"member": flip(member)})
                    w_stages.append((pending, stage))
                    pending = stage
                if share_win:
                    stage = relay(grown, rows_of(near, 0, 0, 1 + share_member), {"win": flip(win)})
                    w_stages.append((pending, stage))
                    pending = stage
        held = held + grown
    w_stages.append((pending, []))

    def w_stage(n):
        if n < len(w_stages):
            for copy in w_stages[n][0]:
                copy.wait_recv()
            for copy in w_stages[n][1]:
                copy.start()

    def norm(i):
        pltpu.make_async_copy(pix.at[i], pix.at[i], fetch_recv.at[i]).wait()
        gain = gain_ref[...]
        offset = bias_ref[...]
        for a in range(step):
            values = pix[i, a].astype(jnp.float32)
            average = jnp.mean(values, axis=-1, keepdims=True)
            centred = values - average
            variance = jnp.mean(centred * centred, axis=-1, keepdims=True)
            scaled = centred * lax.rsqrt(variance + 1e-05) * gain + offset
            nrm[0, i, a] = scaled.astype(jnp.bfloat16)

    def send(i):
        for slot in children(0, lanes):
            gather_copy(slot, i).start()

    inner = [k for k in range(1, lanes) if children(k, lanes)]
    inner.sort(key=lambda k: (bin(k).count("1"), -k))

    def forward(i):
        for k in inner:
            gather_copy(k, i).wait_recv()
            for slot in children(k, lanes):
                gather_copy(slot, i).start()

    def project_qkv(i):
        for k in range(1, lanes):
            if not children(k, lanes):
                gather_copy(k, i).wait_recv()
        window, place = i // 4, i % 4
        x = nrm[:, i].reshape(lanes * group, width)
        lane = lax.broadcasted_iota(jnp.int32, (lanes * group, PADDED), 1)
        ones = jnp.where(lane == CHANNEL_PER_PART, 1.0, 0.0).astype(jnp.bfloat16)
        q_extra = extq[i].reshape(lanes * group, PADDED)
        k_extra = extk[i].reshape(lanes * group, PADDED)
        for t, extra in enumerate((q_extra, k_extra, ones)):
            y = jnp.dot(x, wpad[t], preferred_element_type=jnp.float32).astype(jnp.bfloat16)
            for h in range(heads):
                part_y = y[:, h * PADDED : (h + 1) * PADDED] + extra
                qkv[t, window, :, place, :, h * PADDED : (h + 1) * PADDED] = part_y.reshape(
                    lanes, group, PADDED
                )

    def scores_of(window, k, h):
        span = slice(h * PADDED, (h + 1) * PADDED)
        q = qkv[0, window, k, :, :, span].reshape(chunk, PADDED)
        keys = qkv[1, window, :, :, :, span].reshape(lanes * chunk, PADDED)
        return lax.dot_general(
            q, keys, (((1,), (1,)), ((), ())), preferred_element_type=jnp.float32
        )

    def attend(window, k):
        scores = scores_of(window, k, 0)
        for h in range(heads):
            following = scores_of(window, k, h + 1) if h + 1 < heads else None
            tempered = scale_ref[h : h + 1].reshape(1, 1) * (LOG2E / math.sqrt(CHANNEL_PER_PART))
            values = qkv[2, window, :, :, :, h * PADDED : (h + 1) * PADDED].reshape(
                lanes * chunk, PADDED
            )
            row_max = jnp.max(scores, axis=-1, keepdims=True)
            numerators = jnp.exp2((scores - row_max) * tempered).astype(jnp.bfloat16)
            summed = jnp.dot(numerators, values, preferred_element_type=jnp.float32)
            attended = summed / summed[:, CHANNEL_PER_PART : CHANNEL_PER_PART + 1]
            att_out[window, k, :, h * CHANNEL_PER_PART : (h + 1) * CHANNEL_PER_PART] = attended[
                :, :CHANNEL_PER_PART
            ].astype(jnp.bfloat16)
            scores = following

    def attend_and_send(window, k):
        attend(window, k)

        @pl.when(k > 0)
        def _():
            attended_copy(window, k).start()

    tile = 512 if width % 512 == 0 else width

    def store(window, columns, total):
        total = total.astype(jnp.bfloat16).reshape(4, step, HALF, tile)
        for piece in range(4):
            first = window * WS + (piece % 2) * HALF
            start = (piece // 2) * step
            out_ref[0, start : start + step, 0, first : first + HALF, columns] = total[piece]

    def residual(window, columns):
        return pix[window * 4 : window * 4 + 4, :, :, columns].reshape(chunk, tile).astype(jnp.float32)

    def project_out(window, ready, late):
        for start in range(0, width, tile):
            columns = slice(start, start + tile)
            total = residual(window, columns)
            for k in ready:
                source_ref = att_out if k == 0 else att_in
                total += jnp.dot(
                    source_ref[window, k], wall[k, :, columns], preferred_element_type=jnp.float32
                )
            if late:
                acc[:, columns] = total
            else:
                store(window, columns, total)
        for n, k in enumerate(late):
            attended_copy(window, k).wait_recv()
            for start in range(0, width, tile):
                columns = slice(start, start + tile)
                total = acc[:, columns] + jnp.dot(
                    att_in[window, k], wall[k, :, columns], preferred_element_type=jnp.float32
                )
                if n + 1 < len(late):
                    acc[:, columns] = total
                else:
                    store(window, columns, total)

    barrier = pltpu.get_barrier_semaphore()
    line = blocks == 4
    greeted = [{"win": flip(win)}] if line else [{"win": (win + 2) % blocks}, {"win": flip(win)}]
    greeted += [at_seq(k) for k in reversed(range(1, lanes))]
    if share_far and blocks != 4:
        greeted.append({"win": flip(win, 2)})
    if share_member:
        greeted.append({"member": flip(member)})
    for device in greeted:
        pl.semaphore_signal(barrier, inc=1, device_id=device, device_id_type=MESH)
    if line:
        beside = win + 2 * (win % 2) - 1
        middle = ((win + 1) // 2) % 2

        @pl.when(middle == 1)
        def _():
            pl.semaphore_signal(barrier, inc=1, device_id={"win": beside}, device_id_type=MESH)

    for copy in locals_:
        copy.start()
    loads = [
        pltpu.make_async_copy(src, dst, local_sem.at[n])
        for n, (src, dst) in enumerate(
            [
                (gain_hbm, gain_ref),
                (bias_hbm, bias_ref),
                (label_hbm, label_ref),
                (scale_hbm, scale_ref),
                (wqkv_ref, raw),
                (wout_ref, wall.at[0]),
            ]
        )
    ]
    for copy in loads:
        copy.start()
    loads[0].wait()
    loads[1].wait()

    @pl.loop(0, 2)
    def _(i):
        norm(i)

    pl.semaphore_wait(barrier, len(greeted) + (middle if line else 0))
    send(0)
    if line:

        @pl.when(middle == 1)
        def _():
            for device in ({"win": beside}, {"win": flip(win)}):
                pl.semaphore_signal(near_sem, inc=1, device_id=device, device_id_type=MESH)

    for copy in fetches[:2]:
        copy.start()
    w_stage(0)
    send(1)
    if line:
        pl.semaphore_wait(near_sem, 1)
    pl.semaphore_signal(
        known_sem, inc=1, device_id={"win": (win + 2) % blocks}, device_id_type=MESH
    )
    for copy in fetches[2:]:
        copy.start()
    norm(4)
    pl.semaphore_wait(known_sem, 1)
    for copy in corners:
        copy.start()

    labt[...] = jnp.zeros_like(labt)
    loads[2].wait()
    for k in range(lanes):
        lane_of = xor(me, k, bits)
        for a in range(rows):
            labt[a : a + 1, :cols] = label_ref[0, pl.ds(a * lanes + lane_of, 1), :].astype(jnp.float32)
        turned = jnp.transpose(labt[...])
        for i in range(pieces):
            first = (i // 4) * WS + (i % 2) * HALF
            for a in range(step):
                row = ((i // 2) % 2) * step + a
                label = turned[first : first + HALF, row : row + 1].astype(jnp.int32)
                lane = lax.broadcasted_iota(jnp.int32, (HALF, PADDED), 1) - CHANNEL_PER_PART
                same = lane == label
                extq[i, k, a] = jnp.where(same, 1.0, 0.0).astype(jnp.bfloat16)
                extk[i, k, a] = jnp.where(
                    jnp.logical_and(lane >= 0, jnp.logical_not(same)), -1e30, 0.0
                ).astype(jnp.bfloat16)

    loads[3].wait()
    loads[4].wait()
    tall = width // 4

    @pl.loop(0, 12)
    def _(n):
        t, r = n // 4, pl.multiple_of((n % 4) * tall, tall)
        for h in range(heads):
            part_w = raw[t, pl.ds(r, tall), h * CHANNEL_PER_PART : (h + 1) * CHANNEL_PER_PART]
            empty = jnp.zeros((tall, PADDED - CHANNEL_PER_PART), part_w.dtype)
            wpad[t, pl.ds(r, tall), h * PADDED : (h + 1) * PADDED] = jnp.concatenate(
                [part_w, empty], axis=1
            )

    @pl.loop(2, 4)
    def _(i):
        norm(i)
        send(i)

    w_stage(1)

    @pl.loop(0, 4)
    def _(i):
        @pl.when(i > 0)
        def _():
            norm(i + 4)

        send(i + 4)
        forward(i)

        @pl.when(i > 0)
        def _():
            project_qkv(i - 1)

    per = lanes // 4

    @pl.loop(0, 4)
    def _(i):
        forward(i + 4)
        project_qkv(i + 3)

        @pl.when(i == 0)
        def _():
            w_stage(2)

        @pl.when(i == 2)
        def _():
            w_stage(3)

        @pl.when(i < 3)
        def _():
            for n in range(per):
                attend_and_send(0, lanes - 1 - i * per - n)

    project_qkv(pieces - 1)

    @pl.loop(0, 2 * per)
    def _(i):
        attend_and_send(1, lanes - 1 - i)

    for n in range(4, len(w_stages) - 1):
        w_stage(n)

    @pl.loop(0, 3 * per)
    def _(i):
        window = (i + 2 * per) // (3 * per)
        attend_and_send(window, per - 1 - i + 2 * per * window)

    w_stage(max(4, len(w_stages) - 1))
    loads[5].wait()
    for k in reversed(range(1, lanes)):
        attended_copy(0, k).wait_recv()
    project_out(0, list(range(lanes)), [])
    for copy in fetches + corners:
        copy.wait_send()

    @pl.loop(0, pieces)
    def _(i):
        for k in range(1, lanes):
            gather_copy(k, i).wait_send()

    for copy in w_copies:
        copy.wait_send()
    for k in range(1, lanes):
        attended_copy(0, k).wait_send()
    for window in range(1, window_count):
        project_out(window, [0], [1] + list(reversed(range(2, lanes))))

    for window in range(1, window_count):
        for k in range(1, lanes):
            attended_copy(window, k).wait_send()


def share_levels(members, blocks, head_width):
    by_member = int(members == 2 and head_width % 32 == 0)
    by_win = int(by_member and blocks % 2 == 0 and head_width % 64 == 0)
    by_far = int(by_win and blocks % 4 == 0 and head_width % 128 == 0)
    return by_member, by_win, by_far


def on_device(x, labels, gain, offset, wqkv, scale, wout):
    lanes = lax.axis_size("seq")
    blocks = lax.axis_size("win")
    members = lax.axis_size("member")
    _, rows, _, cols, width = x.shape
    step = rows // 2
    window_count = cols // WS
    pieces = 4 * window_count
    head_width = wout.shape[0]
    heads = head_width // CHANNEL_PER_PART
    group = step * HALF
    chunk = 4 * group
    half = jnp.bfloat16
    w_count = 4 * lanes
    in_hbm = functools.partial(pltpu.with_memory_space_constraint, memory_space=pltpu.HBM)
    operands = (scale, x, labels, gain, offset, wqkv, wout)
    return pl.pallas_call(
        functools.partial(layer_kernel, lanes, blocks, members),
        out_shape=pltpu.VMEM(x.shape, x.dtype),
        in_specs=[pl.BlockSpec(memory_space=pltpu.HBM)] * 7,
        out_specs=pl.BlockSpec(memory_space=pltpu.VMEM),
        scratch_shapes=[
            pltpu.VMEM(scale.shape, scale.dtype),
            pltpu.VMEM(labels.shape, labels.dtype),
            pltpu.VMEM(gain.shape, gain.dtype),
            pltpu.VMEM(offset.shape, offset.dtype),
            pltpu.VMEM((pieces, step, HALF, width), half),
            pltpu.VMEM((lanes, pieces, step, HALF, width), half),
            pltpu.VMEM(wqkv.shape, half),
            pltpu.VMEM((3, width, heads * PADDED), half),
            pltpu.VMEM((lanes, head_width, width), half),
            pltpu.VMEM((3, window_count, lanes, 4, group, heads * PADDED), half),
            pltpu.VMEM((pieces, lanes, step, HALF, PADDED), half),
            pltpu.VMEM((pieces, lanes, step, HALF, PADDED), half),
            pltpu.VMEM((8, 128), jnp.float32),
            pltpu.VMEM((window_count, lanes, chunk, head_width), half),
            pltpu.VMEM((window_count, lanes, chunk, head_width), half),
            pltpu.VMEM((chunk, width), jnp.float32),
            pltpu.SemaphoreType.DMA((pieces,)),
            pltpu.SemaphoreType.DMA((pieces,)),
            pltpu.SemaphoreType.DMA((lanes, pieces)),
            pltpu.SemaphoreType.DMA((lanes, pieces)),
            pltpu.SemaphoreType.DMA((window_count, lanes)),
            pltpu.SemaphoreType.DMA((window_count, lanes)),
            pltpu.SemaphoreType.DMA((w_count,)),
            pltpu.SemaphoreType.DMA((w_count,)),
            pltpu.SemaphoreType.DMA((6,)),
            pltpu.SemaphoreType.REGULAR,
            pltpu.SemaphoreType.REGULAR,
        ],
        compiler_params=pltpu.CompilerParams(
            collective_id=0, has_side_effects=True, vmem_limit_bytes=42 << 20
        ),
    )(*[in_hbm(o) if o.size > 1 else o for o in operands])


def solution(mesh):
    in_specs = (
        P(("member", "win"), None, "seq", None, None),
        P(("member", "win"), None, None),
        P(),
        P(),
        P(None, None, "seq"),
        P("seq"),
        P("seq", None),
    )
    out_specs = P(("member", "win"), None, "seq", None, None)
    return jax.shard_map(
        on_device, mesh=mesh, in_specs=in_specs, out_specs=out_specs, check_vma=False
    )
```

```python
import functools
import math

import jax
import jax.numpy as jnp
from jax import lax
from jax.experimental import pallas as pl
from jax.experimental.pallas import tpu as pltpu
from jax.sharding import PartitionSpec as P

CHANNEL_PER_PART = 96
PADDED = 128
WS = 32
HALF = WS // 2
LOG2E = 1.4426950408889634
MESH = pl.DeviceIdType.MESH


def xor(value, mask, bits):
    both = 0
    for b in range(bits):
        both = both + (1 << b) * ((value // (1 << b)) % 2) * ((mask // (1 << b)) % 2)
    return value + mask - 2 * both


def flip(value, bit=1):
    return value + bit - 2 * bit * ((value // bit) % 2)


def children(slot, lanes):
    low = lanes if slot == 0 else slot & -slot
    masks = [1 << b for b in reversed(range(lanes.bit_length() - 1))]
    return [slot | m for m in masks if m < low]


def layer_kernel(
    lanes,
    blocks,
    members,
    scale_hbm,
    x_ref,
    label_hbm,
    gain_hbm,
    bias_hbm,
    wqkv_ref,
    wout_ref,
    out_ref,
    scale_ref,
    label_ref,
    gain_ref,
    bias_ref,
    pix,
    nrm,
    raw,
    wpad,
    wall,
    qkv,
    extq,
    extk,
    labt,
    att_out,
    att_in,
    acc,
    fetch_send,
    fetch_recv,
    norm_send,
    norm_recv,
    att_send,
    att_recv,
    w_send,
    w_recv,
    local_sem,
    known_sem,
    near_sem,
):
    me = lax.axis_index("seq")
    win = lax.axis_index("win")
    member = lax.axis_index("member")
    bits = lanes.bit_length() - 1
    pieces, step, _, width = pix.shape
    rows = 2 * step
    group = step * HALF
    chunk = 4 * group
    window_count = pieces // 4
    head_width = att_out.shape[3]
    heads = head_width // CHANNEL_PER_PART
    cols = window_count * WS

    def at_seq(mask):
        return {"seq": xor(me, mask, bits)}

    def source(i):
        window, place, side = i // 4, (i // 2) % 2, i % 2
        first = window * WS + HALF + side * HALF
        span = pl.ds(step, step) if place == 0 else pl.ds(0, step)
        return place, first, x_ref.at[0, span, 0, pl.ds(first % cols, HALF), :]

    west = (win + blocks - 2) % blocks
    fetches = []
    corners = []
    locals_ = []

    def fetch_copy(src, dst, n, to):
        return pltpu.make_async_remote_copy(
            src_ref=src,
            dst_ref=dst,
            send_sem=fetch_send.at[n],
            recv_sem=fetch_recv.at[n],
            device_id={"win": to},
            device_id_type=MESH,
        )

    for i in range(pieces):
        place, first, src = source(i)
        if place == 0 and first < cols:
            locals_.append(pltpu.make_async_copy(src, pix.at[i], fetch_recv.at[i]))
            continue
        if place == 1 and first >= cols:
            corners.append(fetch_copy(src, pix.at[i], i, flip(west)))
        else:
            fetches.append(fetch_copy(src, pix.at[i], i, flip(win) if place else west))

    def gather_copy(slot, i):
        parent = slot & (slot - 1)
        return pltpu.make_async_remote_copy(
            src_ref=nrm.at[parent, i],
            dst_ref=nrm.at[slot, i],
            send_sem=norm_send.at[slot, i],
            recv_sem=norm_recv.at[slot, i],
            device_id=at_seq(slot ^ parent),
            device_id_type=MESH,
        )

    def attended_copy(window, k, side):
        rows_sent = pl.ds(side * (chunk // 2), chunk // 2)
        return pltpu.make_async_remote_copy(
            src_ref=att_out.at[window, k, rows_sent, :],
            dst_ref=att_in.at[window, k, rows_sent, :],
            send_sem=att_send.at[window, k, side],
            recv_sem=att_recv.at[window, k, side],
            device_id=at_seq(k),
            device_id_type=MESH,
        )

    w_copies = []

    def w_copy(src, dst, device):
        n = len(w_copies)
        copy = pltpu.make_async_remote_copy(
            src_ref=src,
            dst_ref=dst,
            send_sem=w_send.at[n],
            recv_sem=w_recv.at[n],
            device_id=device,
            device_id_type=MESH,
        )
        w_copies.append(copy)
        return copy

    def slot_rows(slot, start, count):
        if slot == 0:
            return wout_ref.at[pl.ds(start, count), :]
        return wall.at[slot, pl.ds(start, count), :]

    share_member, share_win, share_far = share_levels(members, blocks, head_width)
    part = head_width // (1 + share_member) // (1 + share_win) // (1 + share_far)
    near, far = (win % 2) * share_win, ((win // 2) % 2) * share_far
    mine = member * share_member

    def rows_of(b, a, m, count=1):
        start = (((b * (1 + share_far)) + a) * (1 + share_member) + m) * part
        if not isinstance(start, int):
            start = pl.multiple_of(start, 16)
        return start, count * part

    def relay(slots, place, device):
        return [
            w_copy(wall.at[k, pl.ds(*place), :], wall.at[k, pl.ds(*place), :], device)
            for k in slots
        ]

    w_stages = []
    held = [0]
    pending = []
    for mask in [1 << b for b in reversed(range(bits))]:
        grown = [k | mask for k in held]
        if mask == 1:
            direct = [w_copy(slot_rows(0, 0, head_width), wall.at[1], at_seq(1))]
            last = [w_copy(wall.at[k], wall.at[k | 1], at_seq(1)) for k in held if k]
            if w_stages:
                w_stages[0] = (w_stages[0][0], w_stages[0][1] + direct)
                w_stages.append((pending, last))
            else:
                w_stages.append(([], direct))
            pending = last + direct
        else:
            place = rows_of(near, far, mine)
            stage = [
                w_copy(slot_rows(k, *place), wall.at[k | mask, pl.ds(*place), :], at_seq(mask))
                for k in held
            ]
            w_stages.append((pending, stage))
            pending = stage
            if share_far:
                other = 1 - far
                up = relay(grown, place, {"member": flip(member)})
                over = relay(grown, place, {"win": flip(win, 2)})
                w_stages.append((pending, up + over))
                across = relay(grown, rows_of(near, other, mine), {"member": flip(member)})
                batch = relay(grown, rows_of(near, far, 0, 2), {"win": flip(win)})
                batch += relay(grown, rows_of(near, other, mine), {"win": flip(win)})
                w_stages.append((up + over, across + batch))
                rest = relay(grown, rows_of(near, other, 1 - mine), {"win": flip(win)})
                w_stages.append((across, rest))
                pending = batch + rest
            else:
                if share_member:
                    stage = relay(grown, place, {"member": flip(member)})
                    w_stages.append((pending, stage))
                    pending = stage
                if share_win:
                    stage = relay(grown, rows_of(near, 0, 0, 1 + share_member), {"win": flip(win)})
                    w_stages.append((pending, stage))
                    pending = stage
        held = held + grown
    w_stages.append((pending, []))

    def w_stage(n):
        if n < len(w_stages):
            for copy in w_stages[n][0]:
                copy.wait_recv()
            for copy in w_stages[n][1]:
                copy.start()

    def norm(i):
        pltpu.make_async_copy(pix.at[i], pix.at[i], fetch_recv.at[i]).wait()
        gain = gain_ref[...]
        offset = bias_ref[...]
        for a in range(step):
            values = pix[i, a].astype(jnp.float32)
            average = jnp.mean(values, axis=-1, keepdims=True)
            centred = values - average
            variance = jnp.mean(centred * centred, axis=-1, keepdims=True)
            scaled = centred * lax.rsqrt(variance + 1e-05) * gain + offset
            nrm[0, i, a] = scaled.astype(jnp.bfloat16)

    def send(i):
        for slot in children(0, lanes):
            gather_copy(slot, i).start()

    inner = [k for k in range(1, lanes) if children(k, lanes)]
    inner.sort(key=lambda k: (bin(k).count("1"), -k))

    def forward(i):
        for k in inner:
            gather_copy(k, i).wait_recv()
            for slot in children(k, lanes):
                gather_copy(slot, i).start()

    def project_qkv(i):
        for k in range(1, lanes):
            if not children(k, lanes):
                gather_copy(k, i).wait_recv()
        window, place = i // 4, i % 4
        x = nrm[:, i].reshape(lanes * group, width)
        lane = lax.broadcasted_iota(jnp.int32, (lanes * group, PADDED), 1)
        ones = jnp.where(lane == CHANNEL_PER_PART, 1.0, 0.0).astype(jnp.bfloat16)
        q_extra = extq[i].reshape(lanes * group, PADDED)
        k_extra = extk[i].reshape(lanes * group, PADDED)
        for t, extra in enumerate((q_extra, k_extra, ones)):
            y = jnp.dot(x, wpad[t], preferred_element_type=jnp.float32).astype(jnp.bfloat16)
            for h in range(heads):
                part_y = y[:, h * PADDED : (h + 1) * PADDED] + extra
                qkv[t, window, :, place, :, h * PADDED : (h + 1) * PADDED] = part_y.reshape(
                    lanes, group, PADDED
                )

    def scores_of(window, k, h):
        span = slice(h * PADDED, (h + 1) * PADDED)
        q = qkv[0, window, k, :, :, span].reshape(chunk, PADDED)
        keys = qkv[1, window, :, :, :, span].reshape(lanes * chunk, PADDED)
        return lax.dot_general(
            q, keys, (((1,), (1,)), ((), ())), preferred_element_type=jnp.float32
        )

    def attend(window, k):
        scores = scores_of(window, k, 0)
        for h in range(heads):
            following = scores_of(window, k, h + 1) if h + 1 < heads else None
            tempered = scale_ref[h : h + 1].reshape(1, 1) * (LOG2E / math.sqrt(CHANNEL_PER_PART))
            values = qkv[2, window, :, :, :, h * PADDED : (h + 1) * PADDED].reshape(
                lanes * chunk, PADDED
            )
            row_max = jnp.max(scores, axis=-1, keepdims=True)
            numerators = jnp.exp2((scores - row_max) * tempered).astype(jnp.bfloat16)
            summed = jnp.dot(numerators, values, preferred_element_type=jnp.float32)
            attended = summed / summed[:, CHANNEL_PER_PART : CHANNEL_PER_PART + 1]
            att_out[window, k, :, h * CHANNEL_PER_PART : (h + 1) * CHANNEL_PER_PART] = attended[
                :, :CHANNEL_PER_PART
            ].astype(jnp.bfloat16)
            scores = following

    def attend_and_send(window, k):
        attend(window, k)

        @pl.when(k > 0)
        def _():
            for side in range(2):
                attended_copy(window, k, side).start()

    tile = 512 if width % 512 == 0 else width

    def store(window, columns, total, begin=0):
        count = total.shape[0] // group
        total = total.astype(jnp.bfloat16).reshape(count, step, HALF, tile)
        for piece in range(begin, begin + count):
            first = window * WS + (piece % 2) * HALF
            start = (piece // 2) * step
            out_ref[0, start : start + step, 0, first : first + HALF, columns] = total[piece - begin]

    def residual(window, columns):
        return pix[window * 4 : window * 4 + 4, :, :, columns].reshape(chunk, tile).astype(jnp.float32)

    def project_out(window, ready, late):
        for start in range(0, width, tile):
            columns = slice(start, start + tile)
            total = residual(window, columns)
            for k in ready:
                source_ref = att_out if k == 0 else att_in
                total += jnp.dot(
                    source_ref[window, k], wall[k, :, columns], preferred_element_type=jnp.float32
                )
            if late:
                acc[:, columns] = total
            else:
                store(window, columns, total)
        for n, (k, side) in enumerate([(k, side) for k in late for side in range(2)]):
            attended_copy(window, k, side).wait_recv()
            span = slice(side * (chunk // 2), (side + 1) * (chunk // 2))
            for start in range(0, width, tile):
                columns = slice(start, start + tile)
                total = acc[span, columns] + jnp.dot(
                    att_in[window, k, span, :], wall[k, :, columns], preferred_element_type=jnp.float32
                )
                if k != late[-1]:
                    acc[span, columns] = total
                else:
                    store(window, columns, total, 2 * side)

    barrier = pltpu.get_barrier_semaphore()
    line = blocks == 4
    greeted = [{"win": flip(win)}] if line else [{"win": (win + 2) % blocks}, {"win": flip(win)}]
    greeted += [at_seq(k) for k in reversed(range(1, lanes))]
    if share_far and blocks != 4:
        greeted.append({"win": flip(win, 2)})
    if share_member:
        greeted.append({"member": flip(member)})
    for device in greeted:
        pl.semaphore_signal(barrier, inc=1, device_id=device, device_id_type=MESH)
    if line:
        beside = win + 2 * (win % 2) - 1
        middle = ((win + 1) // 2) % 2

        @pl.when(middle == 1)
        def _():
            pl.semaphore_signal(barrier, inc=1, device_id={"win": beside}, device_id_type=MESH)

    for copy in locals_:
        copy.start()
    loads = [
        pltpu.make_async_copy(src, dst, local_sem.at[n])
        for n, (src, dst) in enumerate(
            [
                (gain_hbm, gain_ref),
                (bias_hbm, bias_ref),
                (label_hbm, label_ref),
                (scale_hbm, scale_ref),
                (wqkv_ref, raw),
                (wout_ref, wall.at[0]),
            ]
        )
    ]
    for copy in loads:
        copy.start()
    loads[0].wait()
    loads[1].wait()

    @pl.loop(0, 2)
    def _(i):
        norm(i)

    pl.semaphore_wait(barrier, len(greeted) + (middle if line else 0))
    send(0)
    if line:

        @pl.when(middle == 1)
        def _():
            for device in ({"win": beside}, {"win": flip(win)}):
                pl.semaphore_signal(near_sem, inc=1, device_id=device, device_id_type=MESH)

    for copy in fetches[:2]:
        copy.start()
    w_stage(0)
    send(1)
    if line:
        pl.semaphore_wait(near_sem, 1)
    pl.semaphore_signal(
        known_sem, inc=1, device_id={"win": (win + 2) % blocks}, device_id_type=MESH
    )
    for copy in fetches[2:]:
        copy.start()
    norm(4)
    pl.semaphore_wait(known_sem, 1)
    for copy in corners:
        copy.start()

    labt[...] = jnp.zeros_like(labt)
    loads[2].wait()
    for k in range(lanes):
        lane_of = xor(me, k, bits)
        for a in range(rows):
            labt[a : a + 1, :cols] = label_ref[0, pl.ds(a * lanes + lane_of, 1), :].astype(jnp.float32)
        turned = jnp.transpose(labt[...])
        for i in range(pieces):
            first = (i // 4) * WS + (i % 2) * HALF
            for a in range(step):
                row = ((i // 2) % 2) * step + a
                label = turned[first : first + HALF, row : row + 1].astype(jnp.int32)
                lane = lax.broadcasted_iota(jnp.int32, (HALF, PADDED), 1) - CHANNEL_PER_PART
                same = lane == label
                extq[i, k, a] = jnp.where(same, 1.0, 0.0).astype(jnp.bfloat16)
                extk[i, k, a] = jnp.where(
                    jnp.logical_and(lane >= 0, jnp.logical_not(same)), -1e30, 0.0
                ).astype(jnp.bfloat16)

    loads[3].wait()
    loads[4].wait()
    tall = width // 4

    @pl.loop(0, 12)
    def _(n):
        t, r = n // 4, pl.multiple_of((n % 4) * tall, tall)
        for h in range(heads):
            part_w = raw[t, pl.ds(r, tall), h * CHANNEL_PER_PART : (h + 1) * CHANNEL_PER_PART]
            empty = jnp.zeros((tall, PADDED - CHANNEL_PER_PART), part_w.dtype)
            wpad[t, pl.ds(r, tall), h * PADDED : (h + 1) * PADDED] = jnp.concatenate(
                [part_w, empty], axis=1
            )

    @pl.loop(2, 4)
    def _(i):
        norm(i)
        send(i)

    w_stage(1)

    @pl.loop(0, 4)
    def _(i):
        @pl.when(i > 0)
        def _():
            norm(i + 4)

        send(i + 4)
        forward(i)

        @pl.when(i > 0)
        def _():
            project_qkv(i - 1)

    per = lanes // 4

    @pl.loop(0, 4)
    def _(i):
        forward(i + 4)
        project_qkv(i + 3)

        @pl.when(i == 0)
        def _():
            w_stage(2)

        @pl.when(i == 2)
        def _():
            w_stage(3)

        @pl.when(i < 3)
        def _():
            for n in range(per):
                attend_and_send(0, lanes - 1 - i * per - n)

    project_qkv(pieces - 1)

    @pl.loop(0, 2 * per)
    def _(i):
        attend_and_send(1, lanes - 1 - i)

    for n in range(4, len(w_stages) - 1):
        w_stage(n)

    @pl.loop(0, 3 * per)
    def _(i):
        window = (i + 2 * per) // (3 * per)
        attend_and_send(window, per - 1 - i + 2 * per * window)

    w_stage(max(4, len(w_stages) - 1))
    loads[5].wait()
    for k in reversed(range(1, lanes)):
        for side in range(2):
            attended_copy(0, k, side).wait_recv()
    project_out(0, list(range(lanes)), [])
    for copy in fetches + corners:
        copy.wait_send()

    @pl.loop(0, pieces)
    def _(i):
        for k in range(1, lanes):
            gather_copy(k, i).wait_send()

    for copy in w_copies:
        copy.wait_send()
    for k in range(1, lanes):
        for side in range(2):
            attended_copy(0, k, side).wait_send()
    for window in range(1, window_count):
        project_out(window, [0], [1] + list(reversed(range(2, lanes))))

    for window in range(1, window_count):
        for k in range(1, lanes):
            for side in range(2):
                attended_copy(window, k, side).wait_send()


def share_levels(members, blocks, head_width):
    by_member = int(members == 2 and head_width % 32 == 0)
    by_win = int(by_member and blocks % 2 == 0 and head_width % 64 == 0)
    by_far = int(by_win and blocks % 4 == 0 and head_width % 128 == 0)
    return by_member, by_win, by_far


def on_device(x, labels, gain, offset, wqkv, scale, wout):
    lanes = lax.axis_size("seq")
    blocks = lax.axis_size("win")
    members = lax.axis_size("member")
    _, rows, _, cols, width = x.shape
    step = rows // 2
    window_count = cols // WS
    pieces = 4 * window_count
    head_width = wout.shape[0]
    heads = head_width // CHANNEL_PER_PART
    group = step * HALF
    chunk = 4 * group
    half = jnp.bfloat16
    w_count = 4 * lanes
    in_hbm = functools.partial(pltpu.with_memory_space_constraint, memory_space=pltpu.HBM)
    operands = (scale, x, labels, gain, offset, wqkv, wout)
    return pl.pallas_call(
        functools.partial(layer_kernel, lanes, blocks, members),
        out_shape=pltpu.VMEM(x.shape, x.dtype),
        in_specs=[pl.BlockSpec(memory_space=pltpu.HBM)] * 7,
        out_specs=pl.BlockSpec(memory_space=pltpu.VMEM),
        scratch_shapes=[
            pltpu.VMEM(scale.shape, scale.dtype),
            pltpu.VMEM(labels.shape, labels.dtype),
            pltpu.VMEM(gain.shape, gain.dtype),
            pltpu.VMEM(offset.shape, offset.dtype),
            pltpu.VMEM((pieces, step, HALF, width), half),
            pltpu.VMEM((lanes, pieces, step, HALF, width), half),
            pltpu.VMEM(wqkv.shape, half),
            pltpu.VMEM((3, width, heads * PADDED), half),
            pltpu.VMEM((lanes, head_width, width), half),
            pltpu.VMEM((3, window_count, lanes, 4, group, heads * PADDED), half),
            pltpu.VMEM((pieces, lanes, step, HALF, PADDED), half),
            pltpu.VMEM((pieces, lanes, step, HALF, PADDED), half),
            pltpu.VMEM((8, 128), jnp.float32),
            pltpu.VMEM((window_count, lanes, chunk, head_width), half),
            pltpu.VMEM((window_count, lanes, chunk, head_width), half),
            pltpu.VMEM((chunk, width), jnp.float32),
            pltpu.SemaphoreType.DMA((pieces,)),
            pltpu.SemaphoreType.DMA((pieces,)),
            pltpu.SemaphoreType.DMA((lanes, pieces)),
            pltpu.SemaphoreType.DMA((lanes, pieces)),
            pltpu.SemaphoreType.DMA((window_count, lanes, 2)),
            pltpu.SemaphoreType.DMA((window_count, lanes, 2)),
            pltpu.SemaphoreType.DMA((w_count,)),
            pltpu.SemaphoreType.DMA((w_count,)),
            pltpu.SemaphoreType.DMA((6,)),
            pltpu.SemaphoreType.REGULAR,
            pltpu.SemaphoreType.REGULAR,
        ],
        compiler_params=pltpu.CompilerParams(
            collective_id=0, has_side_effects=True, vmem_limit_bytes=42 << 20
        ),
    )(*[in_hbm(o) if o.size > 1 else o for o in operands])


def solution(mesh):
    in_specs = (
        P(("member", "win"), None, "seq", None, None),
        P(("member", "win"), None, None),
        P(),
        P(),
        P(None, None, "seq"),
        P("seq"),
        P("seq", None),
    )
    out_specs = P(("member", "win"), None, "seq", None, None)
    return jax.shard_map(
        on_device, mesh=mesh, in_specs=in_specs, out_specs=out_specs, check_vma=False
    )
```
